32 devices in a mesh: dp: 1 (over z), tp: 4 (over y), fsdp: 8 (over x, core).
Axes of the slice: x: 4, y: 4, z: 1, core: 2. Of those that a mesh axis runs over, the one named last changes fastest.
The devices are a block of a 4x4x8 slice.
Arguments:
- hidden: bfloat16 [8, 1024, 2048], P(('dp', 'fsdp'))
- positions: int32 [1024], replicated
- norm_gain: float32 [2048], P('fsdp')
- w_query: bfloat16 [2048, 2048], P('fsdp', 'tp')
- w_key: bfloat16 [2048, 256], P('fsdp')
- w_value: bfloat16 [2048, 256], P('fsdp')
- w_gate: bfloat16 [2048, 16384], P('fsdp', 'tp')
- w_up: bfloat16 [2048, 16384], P('fsdp', 'tp')
- w_out: bfloat16 [2048, 2048], P('tp', 'fsdp')
- w_down: bfloat16 [16384, 2048], P('tp', 'fsdp')
Outputs:
- output: bfloat16 [8, 1024, 2048], P(('dp', 'fsdp'))
All inputs are finite; a program needn't handle non-finite values.
Results may differ from the reference program's by a relative error of at most 0.00869661.
Values are sent between devices in bfloat16 or wider.
A program may use at most 768 MiB of HBM per device.

```python
import jax
import jax.numpy as jnp
from jax import lax

BATCH_ROWS = 8
SEQ_LEN = 1024
D_MODEL = 2048
N_HEADS = 8
HEAD_DIM = 256
D_FF = 16384


def setup_inputs(seed: int = 0, part: int = 0) -> dict:
    key_list = jax.random.split(jax.random.key(seed), 11)
    row_key = jax.random.fold_in(key_list[0], part)
    d_scale = D_MODEL ** -0.5
    q_width = N_HEADS * HEAD_DIM
    hidden = jax.random.normal(row_key, (BATCH_ROWS, SEQ_LEN, D_MODEL), jnp.float32)
    pos_steps = jax.random.randint(key_list[1], (SEQ_LEN,), 1, 3, dtype=jnp.int32)
    offset = jax.random.randint(key_list[2], (), 0, 1024, dtype=jnp.int32)
    positions = (offset + jnp.cumsum(pos_steps) - pos_steps[0]).astype(jnp.int32)
    norm_gain = jax.random.uniform(key_list[3], (D_MODEL,), jnp.float32, 0.5, 1.5)
    w_query = 2.0 * d_scale * jax.random.normal(key_list[4], (D_MODEL, q_width), jnp.float32)
    w_key = d_scale * jax.random.normal(key_list[5], (D_MODEL, HEAD_DIM), jnp.float32)
    w_value = d_scale * jax.random.normal(key_list[6], (D_MODEL, HEAD_DIM), jnp.float32)
    w_gate = d_scale * jax.random.normal(key_list[7], (D_MODEL, D_FF), jnp.float32)
    w_up = d_scale * jax.random.normal(key_list[8], (D_MODEL, D_FF), jnp.float32)
    w_out = q_width ** -0.5 * jax.random.normal(key_list[9], (q_width, D_MODEL), jnp.float32)
    w_down = D_FF ** -0.5 * jax.random.normal(key_list[10], (D_FF, D_MODEL), jnp.float32)
    return {
        "hidden": hidden.astype(jnp.bfloat16),
        "positions": positions,
        "norm_gain": norm_gain,
        "w_query": w_query.astype(jnp.bfloat16),
        "w_key": w_key.astype(jnp.bfloat16),
        "w_value": w_value.astype(jnp.bfloat16),
        "w_gate": w_gate.astype(jnp.bfloat16),
        "w_up": w_up.astype(jnp.bfloat16),
        "w_out": w_out.astype(jnp.bfloat16),
        "w_down": w_down.astype(jnp.bfloat16),
    }


def rope_tables(positions, head_dim):
    inv_freq = 10000.0 ** (-jnp.arange(0, head_dim, 2, dtype=jnp.float32) / head_dim)
    angles = positions.astype(jnp.float32)[:, None] * inv_freq[None, :]
    angles = jnp.concatenate([angles, angles], axis=-1)
    return jnp.cos(angles), jnp.sin(angles)


def rope_rotate(vectors, cos_t, sin_t):
    half_dim = vectors.shape[-1] // 2
    rotated = jnp.concatenate([-vectors[..., half_dim:], vectors[..., :half_dim]], axis=-1)
    return vectors * cos_t + rotated * sin_t


def layer_norm(hidden, gain_vec):
    row_f32 = hidden.astype(jnp.float32)
    centered = row_f32 - jnp.mean(row_f32, axis=-1, keepdims=True)
    variance = jnp.mean(centered * centered, axis=-1, keepdims=True)
    return (centered * lax.rsqrt(variance + 1e-6) * gain_vec).astype(jnp.bfloat16)


def reference(hidden, positions, norm_gain, w_query, w_key, w_value, w_gate, w_up, w_out, w_down):
    cos_t, sin_t = rope_tables(positions, HEAD_DIM)
    q_block = min(256, SEQ_LEN)
    n_blocks = SEQ_LEN // q_block
    score_scale = HEAD_DIM ** -0.5
    key_index = jnp.arange(SEQ_LEN)

    def seq_layer(seq_rows):
        normed = layer_norm(seq_rows, norm_gain)
        query_raw = jnp.dot(normed, w_query, preferred_element_type=jnp.float32).astype(jnp.bfloat16)
        key_raw = jnp.dot(normed, w_key, preferred_element_type=jnp.float32).astype(jnp.bfloat16)
        values = jnp.dot(normed, w_value, preferred_element_type=jnp.float32).astype(jnp.bfloat16)
        gate_raw = jnp.dot(normed, w_gate, preferred_element_type=jnp.float32).astype(jnp.bfloat16)
        up_raw = jnp.dot(normed, w_up, preferred_element_type=jnp.float32).astype(jnp.bfloat16)
        query_rot = rope_rotate(query_raw.reshape(SEQ_LEN, N_HEADS, HEAD_DIM).astype(jnp.float32), cos_t[:, None, :], sin_t[:, None, :]).astype(jnp.bfloat16)
        key_f32 = rope_rotate(key_raw.astype(jnp.float32), cos_t, sin_t).astype(jnp.bfloat16).astype(jnp.float32)
        value_f32 = values.astype(jnp.float32)
        query_blocks = query_rot.reshape(n_blocks, q_block, N_HEADS, HEAD_DIM)

        def block_attn(block_args):
            query_rows, blk_start = block_args
            scores = jnp.einsum("qhe,te->qht", query_rows.astype(jnp.float32), key_f32) * score_scale
            query_index = blk_start + jnp.arange(q_block)
            causal_mask = key_index[None, None, :] <= query_index[:, None, None]
            scores = jnp.where(causal_mask, scores, -1e30)
            prob_rows = jax.nn.softmax(scores, axis=-1).astype(jnp.bfloat16)
            attn_rows = jnp.einsum("qht,te->qhe", prob_rows.astype(jnp.float32), value_f32)
            return attn_rows.astype(jnp.bfloat16)

        attn_out = lax.map(block_attn, (query_blocks, jnp.arange(n_blocks) * q_block))
        attn_out = attn_out.reshape(SEQ_LEN, N_HEADS * HEAD_DIM)
        gated_act = (jax.nn.silu(gate_raw.astype(jnp.float32)) * up_raw.astype(jnp.float32)).astype(jnp.bfloat16)
        branch = jnp.dot(attn_out, w_out, preferred_element_type=jnp.float32) + jnp.dot(gated_act, w_down, preferred_element_type=jnp.float32)
        return (seq_rows.astype(jnp.float32) + branch).astype(jnp.bfloat16)

    return lax.map(seq_layer, hidden)
```

```python
import functools

import jax
import jax.numpy as jnp
from jax import lax
from jax.experimental import pallas as pl
from jax.experimental.pallas import tpu as pltpu
from jax.sharding import PartitionSpec as P

NORM_EPS = 1e-6
MESH = pl.DeviceIdType.MESH
A, B = 0, 1
OWN, RIGHT, OPP, LEFT = 0, 1, 2, 3
MT = 512


def dot(a, b):
    return jnp.dot(a, b, preferred_element_type=jnp.float32)


def layer_kernel(dims, x, gain, cos, sin, wq, wk, wv, wg, wu, wo, wd,
                 out, land, dland,
                 xv, h, za, stg, act, cosv, sinv, gl, dstg, part, rs1, s1, rs2, ag,
                 r_ici, r_par, s_ici, s_par, r_d, s_d, s_dp, r_y, s_y, r_g, s_g, lsem, dsem, osem):
    seq, dm, rows, qw, hd, ff, tk, cw, nchunk, half = dims
    n_chips = lax.axis_size("fsdp") // 2
    n_dev = lax.axis_size("fsdp")
    me = lax.axis_index("fsdp")
    t = lax.axis_index("tp")
    chip, core = me // 2, me % 2
    other = 1 - core

    def dev(r, c):
        return 2 * lax.rem(chip + r, n_chips) + c

    right, left, partner = dev(RIGHT, core), dev(LEFT, core), dev(OWN, other)

    def remote(src, dst, ssem, rsem, target):
        return pltpu.make_async_remote_copy(src_ref=src, dst_ref=dst, send_sem=ssem, recv_sem=rsem,
                                            device_id=target, device_id_type=MESH)

    def wait_recv(ref, sem):
        remote(ref, ref, sem, sem, {"fsdp": partner}).wait_recv()

    def wait_send(ref, sem):
        remote(ref, ref, sem, sem, {"fsdp": partner}).wait_send()

    barrier = pltpu.get_barrier_semaphore()
    for d in range(1, 8):
        pl.semaphore_signal(barrier, inc=1, device_id={"fsdp": lax.rem(me + d, n_dev)}, device_id_type=MESH)
    for m in (1, 3):
        pl.semaphore_signal(barrier, inc=1, device_id={"tp": t ^ m}, device_id_type=MESH)
    pl.semaphore_wait(barrier, 9)

    def own_parts(n, first):
        if first:
            return ((wq, slice(None), A, 0, qw), (wk, slice(None), B, 0, hd), (wv, slice(None), B, hd, hd))
        col = pl.multiple_of((n - 1) * cw, cw)
        return ((wg, pl.ds(col, cw), A, 0, cw), (wu, pl.ds(col, cw), B, 0, cw))

    def own_send(n, first=False):
        for target, slot, who in ((right, 0, LEFT), (left, 3, RIGHT)):
            for src, cols, ab, off, width in own_parts(n, first):
                remote(src.at[:, cols], land.at[n, me, ab, :, pl.ds(off, width)],
                       s_ici.at[n, slot + ab], r_ici.at[n, who - 1, ab], {"fsdp": target}).start()
        for src, cols, ab, off, width in own_parts(n, first):
            remote(src.at[:, cols], land.at[n, me, ab, :, pl.ds(off, width)],
                   s_par.at[n, OWN, ab], r_par.at[n, OWN, ab], {"fsdp": partner}).start()

    def pass_on(n, r, ab):
        ref = land.at[n, dev(r, core), ab]
        remote(ref, ref, s_par.at[n, r, ab], r_par.at[n, r, ab], {"fsdp": partner}).start()

    def service(n):
        for r, fwd, target, slot in ((LEFT, A, right, 2), (RIGHT, B, left, 5)):
            for ab in (fwd, 1 - fwd):
                ref = land.at[n, dev(r, core), ab]
                wait_recv(ref, r_ici.at[n, r - 1, ab])
                if ab == fwd:
                    remote(ref, ref, s_ici.at[n, slot], r_ici.at[n, OPP - 1, ab], {"fsdp": target}).start()
                pass_on(n, r, ab)

    def finish(n, first=False):
        for ab in (A, B):
            wait_recv(land.at[n, dev(OPP, core), ab], r_ici.at[n, OPP - 1, ab])
            pass_on(n, OPP, ab)
        for src, cols, ab, off, width in own_parts(n, first):
            pltpu.make_async_copy(src.at[:, cols], stg.at[ab, me, :, pl.ds(off, width)], lsem).start()
        for r in (RIGHT, LEFT, OPP):
            for ab in (A, B):
                f = dev(r, core)
                pltpu.make_async_copy(land.at[n, f, ab], stg.at[ab, f], lsem).start()
        for r in (OWN, RIGHT, LEFT, OPP):
            for ab in (A, B):
                f = dev(r, other)
                wait_recv(land.at[n, f, ab], r_par.at[n, r, ab])
                pltpu.make_async_copy(land.at[n, f, ab], stg.at[ab, f], lsem).start()
        pltpu.make_async_copy(stg, stg, lsem).wait()

    kparts = ((0, ((wd, 0, half),), half), (half, ((wd, half, ff - half), (wo, 0, qw)), tk - half))

    def down_region(f, hh, kk):
        lo, _, size = kparts[kk]
        return dland.at[f, hh, pl.ds(lo, size), :]

    def down_own(hh, kk, target, ssem, rsem):
        pos = kparts[kk][0]
        for src, lo, size in kparts[kk][1]:
            remote(src.at[pl.ds(lo, size), pl.ds(hh * 128, 128)], dland.at[me, hh, pl.ds(pos, size), :],
                   ssem, rsem, {"fsdp": target}).start()
            pos += size

    def down_send(hh_right, kk):
        down_own(hh_right, kk, right, s_d.at[0, hh_right, kk], r_d.at[0, LEFT, hh_right, kk])
        hh_left = 1 - hh_right
        down_own(hh_left, kk, left, s_d.at[1, hh_left, kk], r_d.at[0, RIGHT, hh_left, kk])

    def down_pass(r, hh, kk):
        ref = down_region(dev(r, core), hh, kk)
        wait_recv(ref, r_d.at[0, r, hh, kk])
        remote(ref, ref, s_dp.at[r, hh, kk], r_d.at[1, r, hh, kk], {"fsdp": partner}).start()

    def down_forward(kk):
        for r, hh, target, way in ((LEFT, 0, right, 0), (RIGHT, 1, left, 1)):
            ref = down_region(dev(r, core), hh, kk)
            wait_recv(ref, r_d.at[0, r, hh, kk])
            remote(ref, ref, s_d.at[way, 2, kk], r_d.at[0, OPP, hh, kk], {"fsdp": target}).start()
            remote(ref, ref, s_dp.at[r, hh, kk], r_d.at[1, r, hh, kk], {"fsdp": partner}).start()

    for d in range(1, 8):
        f = lax.rem(me + d, n_dev)
        remote(gain, gl.at[me], s_g.at[d - 1], r_g.at[d - 1], {"fsdp": f}).start()
    own_send(0, True)
    own_send(1)
    loads = (pltpu.make_async_copy(x, xv, osem.at[0]), pltpu.make_async_copy(cos, cosv, osem.at[1]),
             pltpu.make_async_copy(sin, sinv, osem.at[2]), pltpu.make_async_copy(gain, gl.at[me], osem.at[3]))
    for cp in loads:
        cp.start()
    for cp in loads:
        cp.wait()
    for d in range(1, 8):
        wait_recv(gl.at[lax.rem(me + n_dev - d, n_dev)], r_g.at[d - 1])

    def norm_tile(i, _):
        rr = pl.ds(pl.multiple_of(i * 128, 128), 128)
        row = xv[rr, :].astype(jnp.float32)
        centered = row - jnp.mean(row, axis=-1, keepdims=True)
        var = jnp.mean(centered * centered, axis=-1, keepdims=True)
        scaled = centered * lax.rsqrt(var + NORM_EPS)
        for f in range(dm // rows):
            cc = slice(f * rows, (f + 1) * rows)
            h[rr, cc] = (scaled[:, cc] * gl[f]).astype(jnp.bfloat16)
        return _

    lax.fori_loop(0, seq // 128, norm_tile, 0)

    def qkv_tile(i, _):
        rr = pl.ds(pl.multiple_of(i * MT, MT), MT)
        hm = h[rr, :]
        cs, sn = cosv[rr, :], sinv[rr, :]
        q = dot(hm, stg[A].reshape(dm, cw)).astype(jnp.bfloat16).astype(jnp.float32)
        kv = dot(hm, stg[B].reshape(dm, cw)).astype(jnp.bfloat16)
        for vec, base in ((q[:, :hd], 0), (q[:, hd:], hd), (kv[:, :hd].astype(jnp.float32), 2 * hd)):
            a, b = vec[:, :hd // 2], vec[:, hd // 2:]
            act[rr, base:base + hd // 2] = (a * cs - b * sn).astype(jnp.bfloat16)
            act[rr, base + hd // 2:base + hd] = (b * cs + a * sn).astype(jnp.bfloat16)
        act[rr, 3 * hd:] = kv[:, hd:]
        return _

    def attention(head):
        qb = 256

        def block(i, _):
            rr = pl.ds(pl.multiple_of(i * qb, qb), qb)
            s = lax.dot_general(act[rr, head * hd:(head + 1) * hd], act[:, 2 * hd:3 * hd],
                                (((1,), (1,)), ((), ())), preferred_element_type=jnp.float32) * (hd ** -0.5)
            qi = i * qb + lax.broadcasted_iota(jnp.int32, (qb, seq), 0)
            ki = lax.broadcasted_iota(jnp.int32, (qb, seq), 1)
            s = jnp.where(ki <= qi, s, -1e30)
            e = jnp.exp(s - jnp.max(s, axis=-1, keepdims=True))
            p = (e * (1.0 / jnp.sum(e, axis=-1, keepdims=True))).astype(jnp.bfloat16)
            o = dot(p, act[:, 3 * hd:])
            za[rr, ff + head * hd:ff + (head + 1) * hd] = o.astype(jnp.bfloat16)
            return _

        lax.fori_loop(0, seq // qb, block, 0)

    def gate_up(n):
        col = pl.ds(pl.multiple_of((n - 1) * cw, cw), cw)

        def tile(i, _):
            rr = pl.ds(pl.multiple_of(i * MT, MT), MT)
            hm = h[rr, :]
            g = dot(hm, stg[A].reshape(dm, cw)).astype(jnp.bfloat16).astype(jnp.float32)
            u = dot(hm, stg[B].reshape(dm, cw)).astype(jnp.bfloat16).astype(jnp.float32)
            za[rr, col] = (g * jax.nn.sigmoid(g) * u).astype(jnp.bfloat16)
            return _

        lax.fori_loop(0, seq // MT, tile, 0)

    service(0)
    own_send(2)
    service(1)
    own_send(3)
    finish(0, True)
    lax.fori_loop(0, seq // MT, qkv_tile, 0)
    for n in (2, 3):
        service(n)
        own_send(n + 2)
        finish(n - 1)
        gate_up(n - 1)
        attention(n - 2)

    def step(n, _):
        service(n)
        own_send(n + 2)
        finish(n - 1)
        gate_up(n - 1)
        return _

    lax.fori_loop(4, nchunk - 2, step, 0)
    for n, kk in ((nchunk - 2, 0), (nchunk - 1, 1)):
        service(n)
        down_send(0, kk)
        for hh in (0, 1):
            down_own(hh, kk, partner, s_dp.at[OWN, hh, kk], r_d.at[1, OWN, hh, kk])
        finish(n - 1)
        gate_up(n - 1)
    down_forward(0)
    down_send(1, 0)
    finish(nchunk - 1)
    gate_up(nchunk - 1)
    down_forward(1)
    down_send(1, 1)

    def unit_blocks(g, cc):
        if g == 0:
            sel = ((OWN, 0), (OWN, 1))
        elif g == 1:
            sel = ((LEFT, 0), (RIGHT, 1))
        elif g == 2:
            sel = ((OPP, 0), (OPP, 1))
        else:
            sel = ((LEFT, 1), (RIGHT, 0))
        return [(r, dev(r, core if cc == 0 else other), hh) for r, hh in sel]

    def unit_load(g, cc):
        for s, (r, f, hh) in enumerate(unit_blocks(g, cc)):
            dst = dstg.at[cc, :, pl.ds(s * 128, 128)]
            if g == 0 and cc == 0:
                cols = pl.ds(hh * 128, 128)
                pltpu.make_async_copy(wd.at[:, cols], dstg.at[cc, pl.ds(0, ff), pl.ds(s * 128, 128)], dsem.at[cc]).start()
                pltpu.make_async_copy(wo.at[:, cols], dstg.at[cc, pl.ds(ff, qw), pl.ds(s * 128, 128)], dsem.at[cc]).start()
            else:
                if cc == 1:
                    for kk in (0, 1):
                        wait_recv(down_region(f, hh, kk), r_d.at[1, r, hh, kk])
                pltpu.make_async_copy(dland.at[f, hh], dst, dsem.at[cc]).start()

    def unit_wait(cc):
        pltpu.make_async_copy(dstg.at[cc], dstg.at[cc], dsem.at[cc]).wait()

    b0, b1 = t % 2, t // 2

    def y_plan(cc):
        if cc == 0:
            return t ^ 1, t ^ 3, (b0 + b1) % 2, b1
        return t ^ 3, t ^ 1, b1, b0

    hs, qs = seq // 2, seq // 4

    def ds_(start, size):
        return pl.ds(pl.multiple_of(start, size), size)

    for g in range(4):
        if g == 2:
            for kk in (0, 1):
                for hh in (0, 1):
                    down_pass(OPP, hh, kk)
        if g == 3:
            for kk in (0, 1):
                down_pass(LEFT, 1, kk)
                down_pass(RIGHT, 0, kk)
        unit_load(g, 0)
        for cc in (0, 1):
            if cc == 0:
                unit_load(g, 1)
            unit_wait(cc)
            u = 2 * g + cc

            def tile(i, _, cc=cc, u=u):
                rr = pl.ds(pl.multiple_of(i * MT, MT), MT)
                part[u, rr, :] = dot(za[rr, :], dstg[cc]).astype(jnp.bfloat16)
                return _

            lax.fori_loop(0, seq // MT, tile, 0)
            p1, p2, k1, k2 = y_plan(cc)
            remote(part.at[u, ds_((1 - k1) * hs, hs), :], rs1.at[u], s_y.at[u, 0], r_y.at[u, 0], {"tp": p1}).start()
        for cc in (0, 1):
            u = 2 * g + cc
            p1, p2, k1, k2 = y_plan(cc)
            wait_recv(rs1.at[u], r_y.at[u, 0])
            s1[u] = (part[u, ds_(k1 * hs, hs), :].astype(jnp.float32) + rs1[u].astype(jnp.float32)).astype(jnp.bfloat16)
            remote(s1.at[u, ds_((1 - k2) * qs, qs), :], rs2.at[u], s_y.at[u, 1], r_y.at[u, 1], {"tp": p2}).start()
        for cc in (0, 1):
            u = 2 * g + cc
            p1, p2, k1, k2 = y_plan(cc)
            wait_recv(rs2.at[u], r_y.at[u, 1])
            rr = ds_(k1 * hs + k2 * qs, qs)
            tot = s1[u, ds_(k2 * qs, qs), :].astype(jnp.float32) + rs2[u].astype(jnp.float32)
            for s, (r, f, hh) in enumerate(unit_blocks(g, cc)):
                res = xv[rr, ds_(f * 256 + hh * 128, 128)].astype(jnp.float32)
                ag[u, rr, s * 128:(s + 1) * 128] = (res + tot[:, s * 128:(s + 1) * 128]).astype(jnp.bfloat16)
            remote(ag.at[u, rr, :], ag.at[u, rr, :], s_y.at[u, 2], r_y.at[u, 2], {"tp": p2}).start()
        for cc in (0, 1):
            u = 2 * g + cc
            p1, p2, k1, k2 = y_plan(cc)
            wait_recv(ag.at[u, ds_(k1 * hs + (1 - k2) * qs, qs), :], r_y.at[u, 2])
            mine = ag.at[u, ds_(k1 * hs, hs), :]
            remote(mine, mine, s_y.at[u, 3], r_y.at[u, 3], {"tp": p1}).start()
        for cc in (0, 1):
            u = 2 * g + cc
            p1, p2, k1, k2 = y_plan(cc)
            wait_recv(ag.at[u, ds_((1 - k1) * hs, hs), :], r_y.at[u, 3])
            for s, (r, f, hh) in enumerate(unit_blocks(g, cc)):
                pltpu.make_async_copy(ag.at[u, :, pl.ds(s * 128, 128)],
                                      out.at[:, ds_(f * 256 + hh * 128, 128)], osem.at[4]).start()

    pltpu.make_async_copy(ag, ag, osem.at[4]).wait()
    for d in range(1, 8):
        wait_send(gl.at[0], s_g.at[d - 1])

    def drain(n, _):
        for j in range(6):
            wait_send(land.at[0, 0, 0], s_ici.at[n, j])
        for r in range(4):
            for ab in (A, B):
                wait_send(land.at[0, 0, 0], s_par.at[n, r, ab])
        return _

    lax.fori_loop(0, nchunk, drain, 0)
    for kk in (0, 1):
        ref = down_region(0, 0, kk)
        for way in (0, 1):
            for j in range(3):
                wait_send(ref, s_d.at[way, j, kk])
        for r in range(4):
            for hh in (0, 1):
                wait_send(ref, s_dp.at[r, hh, kk])
    for u in range(8):
        for st, ref in enumerate((rs1.at[u], rs2.at[u], rs2.at[u], rs1.at[u])):
            wait_send(ref, s_y.at[u, st])


def solution(mesh):
    row_spec = P(("dp", "fsdp"), None, None)

    def local_layer(hidden, positions, norm_gain, w_query, w_key, w_value, w_gate, w_up, w_out, w_down):
        _, seq, dm = hidden.shape
        rows, qw = w_query.shape
        hd = w_key.shape[1]
        ff = w_gate.shape[1]
        n_dev = dm // rows
        cw = qw
        nchunk = 1 + ff // cw
        tk = ff + qw
        half = ff // 2
        inv_freq = 10000.0 ** (-jnp.arange(0, hd, 2, dtype=jnp.float32) / hd)
        angles = positions.astype(jnp.float32)[:, None] * inv_freq[None, :]
        bf, f32 = jnp.bfloat16, jnp.float32
        dma = pltpu.SemaphoreType.DMA
        dims = (seq, dm, rows, qw, hd, ff, tk, cw, nchunk, half)
        anyspec = pl.BlockSpec(memory_space=pl.ANY)
        out, _, _ = pl.pallas_call(
            functools.partial(layer_kernel, dims),
            out_shape=(jax.ShapeDtypeStruct((seq, dm), bf),
                       jax.ShapeDtypeStruct((nchunk, n_dev, 2, rows, cw), bf),
                       jax.ShapeDtypeStruct((n_dev, 2, tk, 128), bf)),
            in_specs=[anyspec] * 11,
            out_specs=(anyspec,) * 3,
            scratch_shapes=[
                pltpu.VMEM((seq, dm), bf),
                pltpu.VMEM((seq, dm), bf),
                pltpu.VMEM((seq, tk), bf),
                pltpu.VMEM((2, n_dev, rows, cw), bf),
                pltpu.VMEM((seq, 4 * hd), bf),
                pltpu.VMEM((seq, hd // 2), f32),
                pltpu.VMEM((seq, hd // 2), f32),
                pltpu.VMEM((n_dev, 1, rows), f32),
                pltpu.VMEM((2, tk, 256), bf),
                pltpu.VMEM((8, seq, 256), bf),
                pltpu.VMEM((8, seq // 2, 256), bf),
                pltpu.VMEM((8, seq // 2, 256), bf),
                pltpu.VMEM((8, seq // 4, 256), bf),
                pltpu.VMEM((8, seq, 256), bf),
                dma((nchunk, 3, 2)), dma((nchunk, 4, 2)), dma((nchunk, 6)), dma((nchunk, 4, 2)),
                dma((2, 4, 2, 2)), dma((2, 3, 2)), dma((4, 2, 2)),
                dma((8, 4)), dma((8, 4)), dma((7,)), dma((7,)), dma, dma((2,)), dma((5,)),
            ],
            compiler_params=pltpu.CompilerParams(collective_id=0, has_side_effects=True,
                                                 vmem_limit_bytes=67043328),
        )(hidden.reshape(seq, dm), norm_gain.reshape(1, rows), jnp.cos(angles), jnp.sin(angles),
          w_query, w_key, w_value, w_gate, w_up, w_out, w_down)
        return out.reshape(hidden.shape)

    in_specs = (row_spec, P(None), P("fsdp"), P("fsdp", "tp"), P("fsdp", None), P("fsdp", None), P("fsdp", "tp"), P("fsdp", "tp"), P("tp", "fsdp"), P("tp", "fsdp"))
    return jax.shard_map(local_layer, mesh=mesh, in_specs=in_specs, out_specs=row_spec, check_vma=False)
```

```python
import functools

import jax
import jax.numpy as jnp
from jax import lax
from jax.experimental import pallas as pl
from jax.experimental.pallas import tpu as pltpu
from jax.sharding import PartitionSpec as P

NORM_EPS = 1e-6
MESH = pl.DeviceIdType.MESH
A, B = 0, 1
OWN, RIGHT, OPP, LEFT = 0, 1, 2, 3
MT = 512


def dot(a, b):
    return jnp.dot(a, b, preferred_element_type=jnp.float32)


def layer_kernel(dims, x, gain, cos, sin, wq, wk, wv, wg, wu, wo, wd,
                 out, land, dland,
                 xv, h, za, stg, act, cosv, sinv, gl, dstg, part, rs1, s1, rs2, ag,
                 r_ici, r_par, s_ici, s_par, r_d, s_d, s_dp, r_y, s_y, r_g, s_g, lsem, dsem, osem):
    seq, dm, rows, qw, hd, ff, tk, cw, nchunk, half = dims
    n_chips = lax.axis_size("fsdp") // 2
    n_dev = lax.axis_size("fsdp")
    me = lax.axis_index("fsdp")
    t = lax.axis_index("tp")
    chip, core = me // 2, me % 2
    other = 1 - core

    def dev(r, c):
        return 2 * lax.rem(chip + r, n_chips) + c

    right, left, partner = dev(RIGHT, core), dev(LEFT, core), dev(OWN, other)

    def remote(src, dst, ssem, rsem, target):
        return pltpu.make_async_remote_copy(src_ref=src, dst_ref=dst, send_sem=ssem, recv_sem=rsem,
                                            device_id=target, device_id_type=MESH)

    def wait_recv(ref, sem):
        remote(ref, ref, sem, sem, {"fsdp": partner}).wait_recv()

    def wait_send(ref, sem):
        remote(ref, ref, sem, sem, {"fsdp": partner}).wait_send()

    barrier = pltpu.get_barrier_semaphore()
    for d in range(1, 8):
        pl.semaphore_signal(barrier, inc=1, device_id={"fsdp": lax.rem(me + d, n_dev)}, device_id_type=MESH)
    for m in (1, 3):
        pl.semaphore_signal(barrier, inc=1, device_id={"tp": t ^ m}, device_id_type=MESH)
    pl.semaphore_wait(barrier, 9)

    def own_parts(n, first):
        if first:
            return ((wq, slice(None), A, 0, qw), (wk, slice(None), B, 0, hd), (wv, slice(None), B, hd, hd))
        col = pl.multiple_of((n - 1) * cw, cw)
        return ((wg, pl.ds(col, cw), A, 0, cw), (wu, pl.ds(col, cw), B, 0, cw))

    def own_send(n, first=False):
        for target, slot, who in ((right, 0, LEFT), (left, 3, RIGHT)):
            for src, cols, ab, off, width in own_parts(n, first):
                remote(src.at[:, cols], land.at[n, me, ab, :, pl.ds(off, width)],
                       s_ici.at[n, slot + ab], r_ici.at[n, who - 1, ab], {"fsdp": target}).start()
        for src, cols, ab, off, width in own_parts(n, first):
            remote(src.at[:, cols], land.at[n, me, ab, :, pl.ds(off, width)],
                   s_par.at[n, OWN, ab], r_par.at[n, OWN, ab], {"fsdp": partner}).start()

    def pass_on(n, r, ab):
        ref = land.at[n, dev(r, core), ab]
        remote(ref, ref, s_par.at[n, r, ab], r_par.at[n, r, ab], {"fsdp": partner}).start()

    def service(n):
        for r, fwd, target, slot in ((LEFT, A, right, 2), (RIGHT, B, left, 5)):
            for ab in (fwd, 1 - fwd):
                ref = land.at[n, dev(r, core), ab]
                wait_recv(ref, r_ici.at[n, r - 1, ab])
                if ab == fwd:
                    remote(ref, ref, s_ici.at[n, slot], r_ici.at[n, OPP - 1, ab], {"fsdp": target}).start()
                pass_on(n, r, ab)

    def finish(n, first=False):
        for ab in (A, B):
            wait_recv(land.at[n, dev(OPP, core), ab], r_ici.at[n, OPP - 1, ab])
            pass_on(n, OPP, ab)
        for src, cols, ab, off, width in own_parts(n, first):
            pltpu.make_async_copy(src.at[:, cols], stg.at[ab, me, :, pl.ds(off, width)], lsem).start()
        for r in (RIGHT, LEFT, OPP):
            for ab in (A, B):
                f = dev(r, core)
                pltpu.make_async_copy(land.at[n, f, ab], stg.at[ab, f], lsem).start()
        for r in (OWN, RIGHT, LEFT, OPP):
            for ab in (A, B):
                f = dev(r, other)
                wait_recv(land.at[n, f, ab], r_par.at[n, r, ab])
                pltpu.make_async_copy(land.at[n, f, ab], stg.at[ab, f], lsem).start()
        pltpu.make_async_copy(stg, stg, lsem).wait()

    kparts = ((0, ((wd, 0, half),), half), (half, ((wd, half, ff - half), (wo, 0, qw)), tk - half))

    def down_region(f, hh, kk):
        lo, _, size = kparts[kk]
        return dland.at[f, hh, pl.ds(lo, size), :]

    def down_own(hh, kk, target, ssem, rsem):
        pos = kparts[kk][0]
        for src, lo, size in kparts[kk][1]:
            remote(src.at[pl.ds(lo, size), pl.ds(hh * 128, 128)], dland.at[me, hh, pl.ds(pos, size), :],
                   ssem, rsem, {"fsdp": target}).start()
            pos += size

    def down_send(hh_right, kk):
        down_own(hh_right, kk, right, s_d.at[0, hh_right, kk], r_d.at[0, LEFT, hh_right, kk])
        hh_left = 1 - hh_right
        down_own(hh_left, kk, left, s_d.at[1, hh_left, kk], r_d.at[0, RIGHT, hh_left, kk])

    def down_pass(r, hh, kk):
        ref = down_region(dev(r, core), hh, kk)
        wait_recv(ref, r_d.at[0, r, hh, kk])
        remote(ref, ref, s_dp.at[r, hh, kk], r_d.at[1, r, hh, kk], {"fsdp": partner}).start()

    def down_forward(kk):
        for r, hh, target, way in ((LEFT, 0, right, 0), (RIGHT, 1, left, 1)):
            ref = down_region(dev(r, core), hh, kk)
            wait_recv(ref, r_d.at[0, r, hh, kk])
            remote(ref, ref, s_d.at[way, 2, kk], r_d.at[0, OPP, hh, kk], {"fsdp": target}).start()
            remote(ref, ref, s_dp.at[r, hh, kk], r_d.at[1, r, hh, kk], {"fsdp": partner}).start()

    for d in range(1, 8):
        f = lax.rem(me + d, n_dev)
        remote(gain, gl.at[me], s_g.at[d - 1], r_g.at[d - 1], {"fsdp": f}).start()
    own_send(0, True)
    own_send(1)
    loads = (pltpu.make_async_copy(x, xv, osem.at[0]), pltpu.make_async_copy(cos, cosv, osem.at[1]),
             pltpu.make_async_copy(sin, sinv, osem.at[2]), pltpu.make_async_copy(gain, gl.at[me], osem.at[3]))
    for cp in loads:
        cp.start()
    for cp in loads:
        cp.wait()
    for d in range(1, 8):
        wait_recv(gl.at[lax.rem(me + n_dev - d, n_dev)], r_g.at[d - 1])

    def norm_tile(i, _):
        rr = pl.ds(pl.multiple_of(i * 128, 128), 128)
        row = xv[rr, :].astype(jnp.float32)
        centered = row - jnp.mean(row, axis=-1, keepdims=True)
        var = jnp.mean(centered * centered, axis=-1, keepdims=True)
        scaled = centered * lax.rsqrt(var + NORM_EPS)
        for f in range(dm // rows):
            cc = slice(f * rows, (f + 1) * rows)
            h[rr, cc] = (scaled[:, cc] * gl[f]).astype(jnp.bfloat16)
        return _

    lax.fori_loop(0, seq // 128, norm_tile, 0)

    def qkv_tile(i, _):
        rr = pl.ds(pl.multiple_of(i * MT, MT), MT)
        hm = h[rr, :]
        cs, sn = cosv[rr, :], sinv[rr, :]
        q = dot(hm, stg[A].reshape(dm, cw)).astype(jnp.bfloat16).astype(jnp.float32)
        kv = dot(hm, stg[B].reshape(dm, cw)).astype(jnp.bfloat16)
        for vec, base in ((q[:, :hd], 0), (q[:, hd:], hd), (kv[:, :hd].astype(jnp.float32), 2 * hd)):
            a, b = vec[:, :hd // 2], vec[:, hd // 2:]
            act[rr, base:base + hd // 2] = (a * cs - b * sn).astype(jnp.bfloat16)
            act[rr, base + hd // 2:base + hd] = (b * cs + a * sn).astype(jnp.bfloat16)
        act[rr, 3 * hd:] = kv[:, hd:]
        return _

    def attention(head):
        qb = 256

        def block(i, _):
            rr = pl.ds(pl.multiple_of(i * qb, qb), qb)
            s = lax.dot_general(act[rr, head * hd:(head + 1) * hd], act[:, 2 * hd:3 * hd],
                                (((1,), (1,)), ((), ())), preferred_element_type=jnp.float32) * (hd ** -0.5)
            qi = i * qb + lax.broadcasted_iota(jnp.int32, (qb, seq), 0)
            ki = lax.broadcasted_iota(jnp.int32, (qb, seq), 1)
            s = jnp.where(ki <= qi, s, -1e30)
            e = jnp.exp(s - jnp.max(s, axis=-1, keepdims=True))
            p = (e * (1.0 / jnp.sum(e, axis=-1, keepdims=True))).astype(jnp.bfloat16)
            o = dot(p, act[:, 3 * hd:])
            za[rr, ff + head * hd:ff + (head + 1) * hd] = o.astype(jnp.bfloat16)
            return _

        lax.fori_loop(0, seq // qb, block, 0)

    def gate_up(n):
        col = pl.ds(pl.multiple_of((n - 1) * cw, cw), cw)

        def tile(i, _):
            rr = pl.ds(pl.multiple_of(i * MT, MT), MT)
            hm = h[rr, :]
            g = dot(hm, stg[A].reshape(dm, cw)).astype(jnp.bfloat16).astype(jnp.float32)
            u = dot(hm, stg[B].reshape(dm, cw)).astype(jnp.bfloat16).astype(jnp.float32)
            za[rr, col] = (g * jax.nn.sigmoid(g) * u).astype(jnp.bfloat16)
            return _

        lax.fori_loop(0, seq // MT, tile, 0)

    service(0)
    own_send(2)
    service(1)
    own_send(3)
    finish(0, True)
    lax.fori_loop(0, seq // MT, qkv_tile, 0)
    for n in (2, 3):
        service(n)
        own_send(n + 2)
        finish(n - 1)
        gate_up(n - 1)
        attention(n - 2)

    def step(n, _):
        service(n)
        own_send(n + 2)
        finish(n - 1)
        gate_up(n - 1)
        return _

    lax.fori_loop(4, nchunk - 2, step, 0)
    for n, kk in ((nchunk - 2, 0), (nchunk - 1, 1)):
        service(n)
        down_send(0, kk)
        for hh in (0, 1):
            down_own(hh, kk, partner, s_dp.at[OWN, hh, kk], r_d.at[1, OWN, hh, kk])
        finish(n - 1)
        gate_up(n - 1)
    down_forward(0)
    down_send(1, 0)
    finish(nchunk - 1)
    gate_up(nchunk - 1)
    down_forward(1)
    down_send(1, 1)

    def unit_blocks(g, cc):
        if g == 0:
            sel = ((OWN, 0), (OWN, 1))
        elif g == 1:
            sel = ((LEFT, 0), (RIGHT, 1))
        elif g == 2:
            sel = ((OPP, 0), (OPP, 1))
        else:
            sel = ((LEFT, 1), (RIGHT, 0))
        return [(r, dev(r, core if cc == 0 else other), hh) for r, hh in sel]

    def unit_load(g, cc):
        for s, (r, f, hh) in enumerate(unit_blocks(g, cc)):
            dst = dstg.at[cc, :, pl.ds(s * 128, 128)]
            if g == 0 and cc == 0:
                cols = pl.ds(hh * 128, 128)
                pltpu.make_async_copy(wd.at[:, cols], dstg.at[cc, pl.ds(0, ff), pl.ds(s * 128, 128)], dsem.at[cc]).start()
                pltpu.make_async_copy(wo.at[:, cols], dstg.at[cc, pl.ds(ff, qw), pl.ds(s * 128, 128)], dsem.at[cc]).start()
            else:
                if cc == 1:
                    for kk in (0, 1):
                        wait_recv(down_region(f, hh, kk), r_d.at[1, r, hh, kk])
                pltpu.make_async_copy(dland.at[f, hh], dst, dsem.at[cc]).start()

    def unit_wait(cc):
        pltpu.make_async_copy(dstg.at[cc], dstg.at[cc], dsem.at[cc]).wait()

    b0, b1 = t % 2, t // 2

    def y_plan(cc):
        if cc == 0:
            return t ^ 1, t ^ 3, (b0 + b1) % 2, b1
        return t ^ 3, t ^ 1, b1, b0

    hs, qs = seq // 2, seq // 4

    def ds_(start, size):
        return pl.ds(pl.multiple_of(start, size), size)

    def compute_unit(g, cc):
        u = 2 * g + cc
        unit_wait(cc)
        p1, _, k1, _ = y_plan(cc)
        for keep in (False, True):
            rr = ds_((k1 if keep else 1 - k1) * hs, hs)
            part[u, rr, :] = dot(za[rr, :], dstg[cc]).astype(jnp.bfloat16)
            if not keep:
                remote(part.at[u, rr, :], rs1.at[u], s_y.at[u, 0], r_y.at[u, 0], {"tp": p1}).start()

    def sum_half(g, cc):
        u = 2 * g + cc
        _, p2, k1, k2 = y_plan(cc)
        wait_recv(rs1.at[u], r_y.at[u, 0])
        s1[u] = (part[u, ds_(k1 * hs, hs), :].astype(jnp.float32) + rs1[u].astype(jnp.float32)).astype(jnp.bfloat16)
        remote(s1.at[u, ds_((1 - k2) * qs, qs), :], rs2.at[u], s_y.at[u, 1], r_y.at[u, 1], {"tp": p2}).start()

    def sum_quarter(g, cc):
        u = 2 * g + cc
        _, p2, k1, k2 = y_plan(cc)
        wait_recv(rs2.at[u], r_y.at[u, 1])
        rr = ds_(k1 * hs + k2 * qs, qs)
        tot = s1[u, ds_(k2 * qs, qs), :].astype(jnp.float32) + rs2[u].astype(jnp.float32)
        for s, (_, f, hh) in enumerate(unit_blocks(g, cc)):
            res = xv[rr, ds_(f * 256 + hh * 128, 128)].astype(jnp.float32)
            ag[u, rr, s * 128:(s + 1) * 128] = (res + tot[:, s * 128:(s + 1) * 128]).astype(jnp.bfloat16)
        remote(ag.at[u, rr, :], ag.at[u, rr, :], s_y.at[u, 2], r_y.at[u, 2], {"tp": p2}).start()

    def share_half(g, cc):
        u = 2 * g + cc
        p1, _, k1, k2 = y_plan(cc)
        wait_recv(ag.at[u, ds_(k1 * hs + (1 - k2) * qs, qs), :], r_y.at[u, 2])
        mine = ag.at[u, ds_(k1 * hs, hs), :]
        remote(mine, mine, s_y.at[u, 3], r_y.at[u, 3], {"tp": p1}).start()

    def store_unit(g, cc):
        u = 2 * g + cc
        _, _, k1, _ = y_plan(cc)
        wait_recv(ag.at[u, ds_((1 - k1) * hs, hs), :], r_y.at[u, 3])
        for s, (_, f, hh) in enumerate(unit_blocks(g, cc)):
            pltpu.make_async_copy(ag.at[u, :, pl.ds(s * 128, 128)],
                                  out.at[:, ds_(f * 256 + hh * 128, 128)], osem.at[4]).start()

    def both(fn, g):
        if 0 <= g < 4:
            fn(g, 0)
            fn(g, 1)

    for g in range(5):
        if g == 2:
            for kk in (0, 1):
                for hh in (0, 1):
                    down_pass(OPP, hh, kk)
        if g == 3:
            for kk in (0, 1):
                down_pass(LEFT, 1, kk)
                down_pass(RIGHT, 0, kk)
        both(unit_load, g if g < 4 else -1)
        both(compute_unit, g if g < 4 else -1)
        both(share_half, g - 1)
        both(sum_half, g)
        both(store_unit, g - 1)
        both(sum_quarter, g)

    pltpu.make_async_copy(ag, ag, osem.at[4]).wait()
    for d in range(1, 8):
        wait_send(gl.at[0], s_g.at[d - 1])

    def drain(n, _):
        for j in range(6):
            wait_send(land.at[0, 0, 0], s_ici.at[n, j])
        for r in range(4):
            for ab in (A, B):
                wait_send(land.at[0, 0, 0], s_par.at[n, r, ab])
        return _

    lax.fori_loop(0, nchunk, drain, 0)
    for kk in (0, 1):
        ref = down_region(0, 0, kk)
        for way in (0, 1):
            for j in range(3):
                wait_send(ref, s_d.at[way, j, kk])
        for r in range(4):
            for hh in (0, 1):
                wait_send(ref, s_dp.at[r, hh, kk])
    for u in range(8):
        for st, ref in enumerate((rs1.at[u], rs2.at[u], rs2.at[u], rs1.at[u])):
            wait_send(ref, s_y.at[u, st])


def solution(mesh):
    row_spec = P(("dp", "fsdp"), None, None)

    def local_layer(hidden, positions, norm_gain, w_query, w_key, w_value, w_gate, w_up, w_out, w_down):
        _, seq, dm = hidden.shape
        rows, qw = w_query.shape
        hd = w_key.shape[1]
        ff = w_gate.shape[1]
        n_dev = dm // rows
        cw = qw
        nchunk = 1 + ff // cw
        tk = ff + qw
        half = ff // 2
        inv_freq = 10000.0 ** (-jnp.arange(0, hd, 2, dtype=jnp.float32) / hd)
        angles = positions.astype(jnp.float32)[:, None] * inv_freq[None, :]
        bf, f32 = jnp.bfloat16, jnp.float32
        dma = pltpu.SemaphoreType.DMA
        dims = (seq, dm, rows, qw, hd, ff, tk, cw, nchunk, half)
        anyspec = pl.BlockSpec(memory_space=pl.ANY)
        out, _, _ = pl.pallas_call(
            functools.partial(layer_kernel, dims),
            out_shape=(jax.ShapeDtypeStruct((seq, dm), bf),
                       jax.ShapeDtypeStruct((nchunk, n_dev, 2, rows, cw), bf),
                       jax.ShapeDtypeStruct((n_dev, 2, tk, 128), bf)),
            in_specs=[anyspec] * 11,
            out_specs=(anyspec,) * 3,
            scratch_shapes=[
                pltpu.VMEM((seq, dm), bf),
                pltpu.VMEM((seq, dm), bf),
                pltpu.VMEM((seq, tk), bf),
                pltpu.VMEM((2, n_dev, rows, cw), bf),
                pltpu.VMEM((seq, 4 * hd), bf),
                pltpu.VMEM((seq, hd // 2), f32),
                pltpu.VMEM((seq, hd // 2), f32),
                pltpu.VMEM((n_dev, 1, rows), f32),
                pltpu.VMEM((2, tk, 256), bf),
                pltpu.VMEM((8, seq, 256), bf),
                pltpu.VMEM((8, seq // 2, 256), bf),
                pltpu.VMEM((8, seq // 2, 256), bf),
                pltpu.VMEM((8, seq // 4, 256), bf),
                pltpu.VMEM((8, seq, 256), bf),
                dma((nchunk, 3, 2)), dma((nchunk, 4, 2)), dma((nchunk, 6)), dma((nchunk, 4, 2)),
                dma((2, 4, 2, 2)), dma((2, 3, 2)), dma((4, 2, 2)),
                dma((8, 4)), dma((8, 4)), dma((7,)), dma((7,)), dma, dma((2,)), dma((5,)),
            ],
            compiler_params=pltpu.CompilerParams(collective_id=0, has_side_effects=True,
                                                 vmem_limit_bytes=67043328),
        )(hidden.reshape(seq, dm), norm_gain.reshape(1, rows), jnp.cos(angles), jnp.sin(angles),
          w_query, w_key, w_value, w_gate, w_up, w_out, w_down)
        return out.reshape(hidden.shape)

    in_specs = (row_spec, P(None), P("fsdp"), P("fsdp", "tp"), P("fsdp", None), P("fsdp", None), P("fsdp", "tp"), P("fsdp", "tp"), P("tp", "fsdp"), P("tp", "fsdp"))
    return jax.shard_map(local_layer, mesh=mesh, in_specs=in_specs, out_specs=row_spec, check_vma=False)
```

```python
import functools

import jax
import jax.numpy as jnp
from jax import lax
from jax.experimental import pallas as pl
from jax.experimental.pallas import tpu as pltpu
from jax.sharding import PartitionSpec as P

NORM_EPS = 1e-6
MESH = pl.DeviceIdType.MESH
A, B = 0, 1
OWN, RIGHT, OPP, LEFT = 0, 1, 2, 3
MT = 512
SLOT = {OWN: 0, RIGHT: 1, LEFT: 0, OPP: 1}


def dot(a, b):
    return jnp.dot(a, b, preferred_element_type=jnp.float32)


def layer_kernel(dims, x, gain, cos, sin, wq, wk, wv, wg, wu, wo, wd,
                 out, lq, lg, ld, lo,
                 h, h2, z, z2, stg, act, cosv, sinv, gl, tr, dstg, part, rs1, s1, rs2, xo, xi, xres, ag,
                 rq, pq, sq, tq, rg, pg, sg, tg, rd, pd, sd, td, ro, po, so, to,
                 sh, rt, sf, rh, sa, ra, r_y, s_y, r_x, s_x, r_gain, s_gain, lsem, dsem, osem):
    seq, dm, rows, qw, hd, ff, qc, kc = dims
    nk = qc // kc
    hs, qs = seq // 2, seq // 4
    n_dev = lax.axis_size("fsdp")
    n_chips = n_dev // 2
    me = lax.axis_index("fsdp")
    t = lax.axis_index("tp")
    chip, core = me // 2, me % 2
    other = 1 - core

    def dev(r, c):
        return 2 * lax.rem(chip + r, n_chips) + c

    right, left, partner, opposite = dev(RIGHT, core), dev(LEFT, core), dev(OWN, other), dev(OPP, core)

    def al(start, size):
        return pl.ds(pl.multiple_of(start, size), size)

    def remote(src, dst, ssem, rsem, target):
        return pltpu.make_async_remote_copy(src_ref=src, dst_ref=dst, send_sem=ssem, recv_sem=rsem,
                                            device_id=target, device_id_type=MESH)

    def send(src, dst, ssem, rsem, f):
        remote(src, dst, ssem, rsem, {"fsdp": f}).start()

    def wait_recv(ref, sem):
        remote(ref, ref, sem, sem, {"fsdp": partner}).wait_recv()

    def wait_send(ref, sem):
        remote(ref, ref, sem, sem, {"fsdp": partner}).wait_send()

    b0, b1 = t % 2, t // 2

    def y_plan(cc):
        if cc == 0:
            return t ^ 1, t ^ 3, (b0 + b1) % 2, b1
        return t ^ 3, t ^ 1, b1, b0

    def my_rows(cc):
        _, _, k1, k2 = y_plan(cc)
        return al(k1 * hs + k2 * qs, qs)

    barrier = pltpu.get_barrier_semaphore()
    for d in range(1, 8):
        pl.semaphore_signal(barrier, inc=1, device_id={"fsdp": lax.rem(me + d, n_dev)}, device_id_type=MESH)
    for m in (1, 3):
        pl.semaphore_signal(barrier, inc=1, device_id={"tp": t ^ m}, device_id_type=MESH)
    pl.semaphore_wait(barrier, 9)

    class Ring:
        def __init__(self, region, own, r, p, s, tp_):
            self.region, self.own, self.r, self.p, self.s, self.t = region, own, r, p, s, tp_

        def own_send(self, ab):
            for way, target, who in ((0, right, LEFT), (1, left, RIGHT)):
                for src, dst in self.own(ab):
                    send(src, dst, self.s.at[way, ab], self.r.at[who - 1, ab], target)
            for src, dst in self.own(ab):
                send(src, dst, self.t.at[OWN, ab], self.p.at[OWN, ab], partner)

        def pass_on(self, r, ab):
            ref = self.region(dev(r, core), ab)
            wait_recv(ref, self.r.at[r - 1, ab])
            send(ref, ref, self.t.at[r, ab], self.p.at[r, ab], partner)

        def service(self):
            for r, ab, target, way in ((LEFT, A, right, 0), (RIGHT, B, left, 1)):
                ref = self.region(dev(r, core), ab)
                wait_recv(ref, self.r.at[r - 1, ab])
                send(ref, ref, self.s.at[way, 2], self.r.at[OPP - 1, ab], target)
                send(ref, ref, self.t.at[r, ab], self.p.at[r, ab], partner)
            self.pass_on(LEFT, B)
            self.pass_on(RIGHT, A)

        def last(self):
            self.pass_on(OPP, A)
            self.pass_on(OPP, B)

        def wait_partner(self, r, ab):
            ref = self.region(dev(r, other), ab)
            wait_recv(ref, self.p.at[r, ab])
            return ref

        def drain(self):
            ref = self.region(0, A)
            for j in range(3):
                for way in (0, 1):
                    wait_send(ref, self.s.at[way, j])
            for r in range(4):
                for ab in (A, B):
                    wait_send(ref, self.t.at[r, ab])

    class Pair:
        def __init__(self, region, own, r, p, s, tp_):
            self.region, self.own, self.r, self.p, self.s, self.t = region, own, r, p, s, tp_

        def one(self, q, side, target, ssem, rsem):
            for src, dst in self.own(lax.rem(chip + q, n_chips), side):
                send(src, dst, ssem, rsem, target)

        def own_send(self):
            self.one(1, 0, right, self.s.at[0, 0], self.r.at[LEFT - 1, 0])
            self.one(2, 1, left, self.s.at[1, 0], self.r.at[RIGHT - 1, 1])
            self.one(0, 1, right, self.s.at[0, 1], self.r.at[LEFT - 1, 1])
            self.one(3, 0, left, self.s.at[1, 1], self.r.at[RIGHT - 1, 0])
            self.one(0, 0, partner, self.t.at[OWN, 0], self.p.at[OWN, 0])
            self.one(3, 1, partner, self.t.at[OWN, 1], self.p.at[OWN, 1])

        def pass_on(self, r, side):
            ref = self.region(dev(r, core), side)
            wait_recv(ref, self.r.at[r - 1, side])
            send(ref, ref, self.t.at[r, side], self.p.at[r, side], partner)

        def forward(self):
            for r, side, target, way in ((LEFT, 0, right, 0), (RIGHT, 1, left, 1)):
                f = dev(r, core)
                ref = self.region(f, side)
                wait_recv(ref, self.r.at[r - 1, side])
                send(ref, self.region(f, 1 - side), self.s.at[way, 2], self.r.at[OPP - 1, 1 - side], target)
                send(ref, ref, self.t.at[r, side], self.p.at[r, side], partner)

        def rest(self):
            self.pass_on(LEFT, 1)
            self.pass_on(RIGHT, 0)

        def service(self):
            self.forward()
            self.rest()

        def last(self):
            self.pass_on(OPP, 0)
            self.pass_on(OPP, 1)

        def wait_partner(self, r, side):
            ref = self.region(dev(r, other), side)
            wait_recv(ref, self.p.at[r, side])
            return ref

        def drain(self):
            ref = self.region(0, 0)
            for j in range(3):
                for way in (0, 1):
                    wait_send(ref, self.s.at[way, j])
            for r in range(4):
                for side in (0, 1):
                    wait_send(ref, self.t.at[r, side])

    def qkv_own(ab):
        if ab == A:
            return ((wq, lq.at[me, A]),)
        return ((wk, lq.at[me, B, :, pl.ds(0, hd)]), (wv, lq.at[me, B, :, pl.ds(hd, hd)]))

    qkv = Ring(lambda f, ab: lq.at[f, ab], qkv_own, rq, pq, sq, tq)

    def o_own(ab):
        return ((wo.at[pl.ds(ab * (qw // 2), qw // 2), :], lo.at[me, ab]),)

    w_o = Ring(lambda f, ab: lo.at[f, ab], o_own, ro, po, so, to)

    def gu(k):
        def own(q, side):
            cols = al(q * qc + k * kc, kc)
            return ((wg.at[:, cols], lg.at[k, side, me, A]), (wu.at[:, cols], lg.at[k, side, me, B]))

        return Pair(lambda f, side: lg.at[k, side, f], own, rg.at[k], pg.at[k], sg.at[k], tg.at[k])

    def d_own(q, side):
        return ((wd.at[al(q * qc, qc), :], ld.at[me, side]),)

    w_d = Pair(lambda f, side: ld.at[f, side], d_own, rd, pd, sd, td)

    def local(src, dst, sem):
        pltpu.make_async_copy(src, dst, sem).start()

    def finish_qkv():
        qkv.last()
        for src, cols, ab, off, width in ((wq, None, A, 0, qw), (wk, None, B, 0, hd), (wv, None, B, hd, hd)):
            local(src, stg.at[ab, me, :, pl.ds(off, width)], lsem)
        for ab in (A, B):
            for r in (RIGHT, LEFT, OPP):
                f = dev(r, core)
                local(lq.at[f, ab], stg.at[ab, f], lsem)
            for r in (OWN, RIGHT, LEFT, OPP):
                local(qkv.wait_partner(r, ab), stg.at[ab, dev(r, other)], lsem)
        pltpu.make_async_copy(stg, stg, lsem).wait()

    def finish_gu(k):
        flow = gu(k)
        flow.last()
        for side in (0, 1):
            cols = pl.ds(side * kc, kc)
            q = lax.rem(chip + 3 * side, n_chips)
            for ab, src in ((A, wg), (B, wu)):
                local(src.at[:, al(q * qc + k * kc, kc)], stg.at[ab, me, :, cols], lsem)
            for r in (RIGHT, LEFT, OPP):
                f = dev(r, core)
                for ab in (A, B):
                    local(lg.at[k, side, f, ab], stg.at[ab, f, :, cols], lsem)
            for r in (OWN, RIGHT, LEFT, OPP):
                f = dev(r, other)
                flow.wait_partner(r, side)
                for ab in (A, B):
                    local(lg.at[k, side, f, ab], stg.at[ab, f, :, cols], lsem)
        pltpu.make_async_copy(stg, stg, lsem).wait()

    hc = dm // 2

    def h_cols(cc):
        return pl.ds(cc * hc, hc)

    def rows_out():
        for cc, target in ((0, right), (1, left)):
            send(h.at[my_rows(cc), h_cols(cc)], tr.at[cc], sh.at[cc], rt.at[cc], target)

    def rows_forward():
        for cc, target in ((0, right), (1, left)):
            wait_recv(tr.at[cc], rt.at[cc])
            send(tr.at[cc], h2.at[my_rows(cc), h_cols(cc)], sf.at[cc], rh.at[cc], target)

    def rows_share(step):
        for cc in (0, 1):
            p1, p2, k1, k2 = y_plan(cc)
            if step == 0:
                mine = h2.at[my_rows(cc), h_cols(cc)]
                wait_recv(mine, rh.at[cc])
                remote(mine, mine, sa.at[cc, 0], ra.at[cc, 0], {"tp": p2}).start()
            elif step == 1:
                wait_recv(h2.at[al(k1 * hs + (1 - k2) * qs, qs), h_cols(cc)], ra.at[cc, 0])
                mine = h2.at[al(k1 * hs, hs), h_cols(cc)]
                remote(mine, mine, sa.at[cc, 1], ra.at[cc, 1], {"tp": p1}).start()
            else:
                wait_recv(h2.at[al((1 - k1) * hs, hs), h_cols(cc)], ra.at[cc, 1])

    def norm_tile(i, _):
        rr = al(i * 128, 128)
        blocks = [ag[f, rr, :].astype(jnp.float32) for f in range(dm // rows)]
        mean = sum(jnp.sum(b, axis=-1, keepdims=True) for b in blocks) * (1.0 / dm)
        cent = [b - mean for b in blocks]
        var = sum(jnp.sum(c * c, axis=-1, keepdims=True) for c in cent) * (1.0 / dm)
        scale = lax.rsqrt(var + NORM_EPS)
        for f in range(dm // rows):
            h[rr, f * rows:(f + 1) * rows] = (cent[f] * scale * gl[f]).astype(jnp.bfloat16)
        return _

    def qkv_tile(i, _):
        rr = al(i * MT, MT)
        hm = h[rr, :]
        cs, sn = cosv[rr, :], sinv[rr, :]
        q = dot(hm, stg[A].reshape(dm, qw)).astype(jnp.bfloat16).astype(jnp.float32)
        kv = dot(hm, stg[B].reshape(dm, qw)).astype(jnp.bfloat16)
        for vec, base in ((q[:, :hd], 0), (q[:, hd:], hd), (kv[:, :hd].astype(jnp.float32), 2 * hd)):
            a, b = vec[:, :hd // 2], vec[:, hd // 2:]
            act[rr, base:base + hd // 2] = (a * cs - b * sn).astype(jnp.bfloat16)
            act[rr, base + hd // 2:base + hd] = (b * cs + a * sn).astype(jnp.bfloat16)
        act[rr, 3 * hd:] = kv[:, hd:]
        return _

    def attention(head):
        qb = 256

        def block(i, _):
            rr = al(i * qb, qb)
            s = lax.dot_general(act[rr, head * hd:(head + 1) * hd], act[:, 2 * hd:3 * hd],
                                (((1,), (1,)), ((), ())), preferred_element_type=jnp.float32) * (hd ** -0.5)
            qi = i * qb + lax.broadcasted_iota(jnp.int32, (qb, seq), 0)
            ki = lax.broadcasted_iota(jnp.int32, (qb, seq), 1)
            s = jnp.where(ki <= qi, s, -1e30)
            e = jnp.exp(s - jnp.max(s, axis=-1, keepdims=True))
            p = (e * (1.0 / jnp.sum(e, axis=-1, keepdims=True))).astype(jnp.bfloat16)
            o = dot(p, act[:, 3 * hd:])
            z[rr, 2 * qc + head * hd:2 * qc + (head + 1) * hd] = o.astype(jnp.bfloat16)
            return _

        lax.fori_loop(0, seq // qb, block, 0)

    def gate_up(k, src, dst):
        def tile(i, _):
            rr = al(i * MT, MT)
            hm = src[rr, :]
            g = dot(hm, stg[A].reshape(dm, 2 * kc)).astype(jnp.bfloat16).astype(jnp.float32)
            u = dot(hm, stg[B].reshape(dm, 2 * kc)).astype(jnp.bfloat16).astype(jnp.float32)
            r = (g * jax.nn.sigmoid(g) * u).astype(jnp.bfloat16)
            for side in (0, 1):
                dst[rr, side * qc + k * kc:side * qc + (k + 1) * kc] = r[:, side * kc:(side + 1) * kc]
            return _

        lax.fori_loop(0, seq // MT, tile, 0)

    def unit_f(g, cc):
        return dev(g, core if cc == 0 else other)

    def group_load(g):
        slot = SLOT[g]
        for cc in (0, 1):
            f = unit_f(g, cc)
            cols = pl.ds(cc * rows, rows)
            for side in (0, 1):
                dst = dstg.at[slot, pl.ds(side * qc, qc), cols]
                if g == OWN and cc == 0:
                    local(wd.at[al(lax.rem(chip + 3 * side, n_chips) * qc, qc), :], dst, dsem.at[slot])
                else:
                    if cc == 1:
                        w_d.wait_partner(g, side)
                    local(ld.at[f, side], dst, dsem.at[slot])
            for ab in (A, B):
                dst = dstg.at[slot, pl.ds(2 * qc + ab * (qw // 2), qw // 2), cols]
                if g == OWN and cc == 0:
                    local(wo.at[pl.ds(ab * (qw // 2), qw // 2), :], dst, dsem.at[slot])
                else:
                    if cc == 1:
                        w_o.wait_partner(g, ab)
                    local(lo.at[f, ab], dst, dsem.at[slot])

    def group_compute(g):
        slot = SLOT[g]
        pltpu.make_async_copy(dstg.at[slot], dstg.at[slot], dsem.at[slot]).wait()
        for s, src, depth in ((1, z2, 2 * qc), (0, z, 2 * qc + qw)):
            def tile(i, _, s=s, src=src, depth=depth):
                rr = al(i * MT, MT)
                r = dot(src[rr, :], dstg[slot, :depth, :]).astype(jnp.bfloat16)
                for cc in (0, 1):
                    part[slot, cc, s, rr, :] = r[:, cc * rows:(cc + 1) * rows]
                return _

            lax.fori_loop(0, seq // MT, tile, 0)
        for cc in (0, 1):
            p1, _, k1, _ = y_plan(cc)
            u = 2 * g + cc
            remote(part.at[slot, cc, :, al((1 - k1) * hs, hs), :], rs1.at[u], s_y.at[u, 0], r_y.at[u, 0], {"tp": p1}).start()

    def sum_half(g):
        for cc in (0, 1):
            _, p2, k1, k2 = y_plan(cc)
            u = 2 * g + cc
            wait_recv(rs1.at[u], r_y.at[u, 0])
            s1[u] = (part[SLOT[g], cc, :, al(k1 * hs, hs), :].astype(jnp.float32) + rs1[u].astype(jnp.float32)).astype(jnp.bfloat16)
            remote(s1.at[u, :, al((1 - k2) * qs, qs), :], rs2.at[u], s_y.at[u, 1], r_y.at[u, 1], {"tp": p2}).start()

    def part_free(g):
        for cc in (0, 1):
            wait_send(rs1.at[0], s_y.at[2 * g + cc, 0])

    def sum_quarter(g):
        for cc in (0, 1):
            _, _, _, k2 = y_plan(cc)
            u = 2 * g + cc
            wait_recv(rs2.at[u], r_y.at[u, 1])
            mine = al(k2 * qs, qs)
            xo[u] = (s1[u, 1, mine, :].astype(jnp.float32) + rs2[u, 1].astype(jnp.float32)).astype(jnp.bfloat16)
            f = unit_f(g, cc)
            send(xo.at[u], xi.at[f], s_x.at[u], r_x.at[f], opposite)

    def close(g):
        for cc in (0, 1):
            _, p2, _, k2 = y_plan(cc)
            u = 2 * g + cc
            f = unit_f(g, cc)
            wait_recv(xi.at[f], r_x.at[f])
            mine = al(k2 * qs, qs)
            tot = s1[u, 0, mine, :].astype(jnp.float32) + rs2[u, 0].astype(jnp.float32) + xi[f].astype(jnp.float32)
            ag[u, my_rows(cc), :] = (xres[u].astype(jnp.float32) + tot).astype(jnp.bfloat16)
            ref = ag.at[u, my_rows(cc), :]
            remote(ref, ref, s_y.at[u, 2], r_y.at[u, 2], {"tp": p2}).start()

    def share_half(g):
        for cc in (0, 1):
            p1, _, k1, k2 = y_plan(cc)
            u = 2 * g + cc
            wait_recv(ag.at[u, al(k1 * hs + (1 - k2) * qs, qs), :], r_y.at[u, 2])
            ref = ag.at[u, al(k1 * hs, hs), :]
            remote(ref, ref, s_y.at[u, 3], r_y.at[u, 3], {"tp": p1}).start()

    def store(g):
        for cc in (0, 1):
            _, _, k1, _ = y_plan(cc)
            u = 2 * g + cc
            wait_recv(ag.at[u, al((1 - k1) * hs, hs), :], r_y.at[u, 3])
            local(ag.at[u], out.at[:, al(unit_f(g, cc) * rows, rows)], osem.at[4])

    for d in range(1, 8):
        f = lax.rem(me + d, n_dev)
        send(gain, gl.at[me], s_gain.at[d - 1], r_gain.at[d - 1], f)
    qkv.own_send(A)
    for f in range(dm // rows):
        local(x.at[:, pl.ds(f * rows, rows)], ag.at[f], osem.at[0])
    local(gain, gl.at[me], osem.at[3])
    local(cos, cosv, osem.at[1])
    local(sin, sinv, osem.at[2])
    pltpu.make_async_copy(ag, ag, osem.at[0]).wait()
    pltpu.make_async_copy(gain, gl.at[me], osem.at[3]).wait()
    for d in range(1, 8):
        wait_recv(gl.at[lax.rem(me + n_dev - d, n_dev)], r_gain.at[d - 1])
    lax.fori_loop(0, seq // 128, norm_tile, 0)
    rows_out()
    qkv.own_send(B)
    rows_forward()
    qkv.service()
    gu(0).own_send()
    gu(1).own_send()
    pltpu.make_async_copy(cos, cosv, osem.at[1]).wait()
    pltpu.make_async_copy(sin, sinv, osem.at[2]).wait()
    rows_share(0)
    finish_qkv()
    lax.fori_loop(0, seq // MT, qkv_tile, 0)
    rows_share(1)
    attention(0)
    gu(0).service()
    gu(2).own_send()
    attention(1)
    finish_gu(0)
    gate_up(0, h, z)
    gu(1).service()
    gu(3).own_send()
    rows_share(2)
    gate_up(0, h2, z2)
    gu(2).service()
    w_o.own_send(A)
    w_o.own_send(B)
    finish_gu(1)
    gate_up(1, h, z)
    gate_up(1, h2, z2)
    gu(3).service()
    w_d.own_send()
    finish_gu(2)
    gate_up(2, h, z)
    gate_up(2, h2, z2)
    w_o.service()
    finish_gu(3)
    gate_up(3, h, z)
    gate_up(3, h2, z2)
    w_d.forward()
    group_load(OWN)
    for g in range(4):
        for cc in (0, 1):
            local(x.at[my_rows(cc), al(unit_f(g, cc) * rows, rows)], xres.at[2 * g + cc], osem.at[0])
    group_compute(OWN)
    w_d.rest()
    w_o.last()
    group_load(RIGHT)
    group_compute(RIGHT)
    sum_half(OWN)
    w_d.last()
    group_load(LEFT)
    part_free(OWN)
    sum_half(RIGHT)
    group_compute(LEFT)
    sum_quarter(OWN)
    group_load(OPP)
    part_free(RIGHT)
    group_compute(OPP)
    pltpu.make_async_copy(xres, xres, osem.at[0]).wait()
    sum_quarter(RIGHT)
    sum_half(LEFT)
    sum_half(OPP)
    sum_quarter(LEFT)
    close(RIGHT)
    close(LEFT)
    sum_quarter(OPP)
    share_half(RIGHT)
    share_half(LEFT)
    close(OPP)
    close(OWN)
    store(RIGHT)
    store(LEFT)
    share_half(OPP)
    share_half(OWN)
    store(OPP)
    store(OWN)

    for d in range(1, 8):
        wait_send(gl.at[0], s_gain.at[d - 1])
    for cc in (0, 1):
        wait_send(tr.at[cc], sh.at[cc])
        wait_send(tr.at[cc], sf.at[cc])
        wait_send(h2.at[pl.ds(0, qs), h_cols(0)], sa.at[cc, 0])
        wait_send(h2.at[pl.ds(0, hs), h_cols(0)], sa.at[cc, 1])
    qkv.drain()
    w_o.drain()
    w_d.drain()
    for k in range(nk):
        gu(k).drain()
    for u in range(8):
        if u // 2 in (LEFT, OPP):
            wait_send(rs1.at[u], s_y.at[u, 0])
        wait_send(rs2.at[u], s_y.at[u, 1])
        wait_send(xo.at[u], s_x.at[u])
        wait_send(ag.at[u, pl.ds(0, qs), :], s_y.at[u, 2])
        wait_send(ag.at[u, pl.ds(0, hs), :], s_y.at[u, 3])
    pltpu.make_async_copy(ag, ag, osem.at[4]).wait()


def solution(mesh):
    row_spec = P(("dp", "fsdp"), None, None)

    def local_layer(hidden, positions, norm_gain, w_query, w_key, w_value, w_gate, w_up, w_out, w_down):
        _, seq, dm = hidden.shape
        rows, qw = w_query.shape
        hd = w_key.shape[1]
        ff = w_gate.shape[1]
        n_dev = dm // rows
        qc = ff // (n_dev // 2)
        kc = qw // 2
        nk = qc // kc
        inv_freq = 10000.0 ** (-jnp.arange(0, hd, 2, dtype=jnp.float32) / hd)
        angles = positions.astype(jnp.float32)[:, None] * inv_freq[None, :]
        bf, f32 = jnp.bfloat16, jnp.float32
        dma = pltpu.SemaphoreType.DMA
        dims = (seq, dm, rows, qw, hd, ff, qc, kc)
        anyspec = pl.BlockSpec(memory_space=pl.ANY)
        out = pl.pallas_call(
            functools.partial(layer_kernel, dims),
            out_shape=(jax.ShapeDtypeStruct((seq, dm), bf),
                       jax.ShapeDtypeStruct((n_dev, 2, rows, qw), bf),
                       jax.ShapeDtypeStruct((nk, 2, n_dev, 2, rows, kc), bf),
                       jax.ShapeDtypeStruct((n_dev, 2, qc, rows), bf),
                       jax.ShapeDtypeStruct((n_dev, 2, qw // 2, rows), bf)),
            in_specs=[anyspec] * 11,
            out_specs=(anyspec,) * 5,
            scratch_shapes=[
                pltpu.VMEM((seq, dm), bf),
                pltpu.VMEM((seq, dm), bf),
                pltpu.VMEM((seq, 2 * qc + qw), bf),
                pltpu.VMEM((seq, 2 * qc), bf),
                pltpu.VMEM((2, n_dev, rows, qw), bf),
                pltpu.VMEM((seq, 4 * hd), bf),
                pltpu.VMEM((seq, hd // 2), f32),
                pltpu.VMEM((seq, hd // 2), f32),
                pltpu.VMEM((n_dev, 1, rows), f32),
                pltpu.VMEM((2, seq // 4, dm // 2), bf),
                pltpu.VMEM((2, 2 * qc + qw, 2 * rows), bf),
                pltpu.VMEM((2, 2, 2, seq, rows), bf),
                pltpu.VMEM((8, 2, seq // 2, rows), bf),
                pltpu.VMEM((8, 2, seq // 2, rows), bf),
                pltpu.VMEM((8, 2, seq // 4, rows), bf),
                pltpu.VMEM((8, seq // 4, rows), bf),
                pltpu.VMEM((8, seq // 4, rows), bf),
                pltpu.VMEM((8, seq // 4, rows), bf),
                pltpu.VMEM((8, seq, rows), bf),
                dma((3, 2)), dma((4, 2)), dma((2, 3)), dma((4, 2)),
                dma((nk, 3, 2)), dma((nk, 4, 2)), dma((nk, 2, 3)), dma((nk, 4, 2)),
                dma((3, 2)), dma((4, 2)), dma((2, 3)), dma((4, 2)),
                dma((3, 2)), dma((4, 2)), dma((2, 3)), dma((4, 2)),
                dma((2,)), dma((2,)), dma((2,)), dma((2,)), dma((2, 2)), dma((2, 2)),
                dma((8, 4)), dma((8, 4)), dma((8,)), dma((8,)), dma((7,)), dma((7,)),
                dma, dma((2,)), dma((5,)),
            ],
            compiler_params=pltpu.CompilerParams(collective_id=0, has_side_effects=True,
                                                 vmem_limit_bytes=67043328),
        )(hidden.reshape(seq, dm), norm_gain.reshape(1, rows), jnp.cos(angles), jnp.sin(angles),
          w_query, w_key, w_value, w_gate, w_up, w_out, w_down)[0]
        return out.reshape(hidden.shape)

    in_specs = (row_spec, P(None), P("fsdp"), P("fsdp", "tp"), P("fsdp", None), P("fsdp", None), P("fsdp", "tp"), P("fsdp", "tp"), P("tp", "fsdp"), P("tp", "fsdp"))
    return jax.shard_map(local_layer, mesh=mesh, in_specs=in_specs, out_specs=row_spec, check_vma=False)
```

```python
import functools

import jax
import jax.numpy as jnp
from jax import lax
from jax.experimental import pallas as pl
from jax.experimental.pallas import tpu as pltpu
from jax.sharding import PartitionSpec as P

NORM_EPS = 1e-6
MESH = pl.DeviceIdType.MESH
A, B = 0, 1
OWN, RIGHT, OPP, LEFT = 0, 1, 2, 3
MT = 512
SLOT = {OWN: 0, RIGHT: 1, LEFT: 0, OPP: 1}


def dot(a, b):
    return jnp.dot(a, b, preferred_element_type=jnp.float32)


def layer_kernel(dims, x, gain, pos, freq, wq, wk, wv, wg, wu, wo, wd,
                 out, lq, lg, ld, lo,
                 h, h2, z, z2, stg, act, posv, freqv, cosv, sinv, gl, tr, dstg, part, rs1, s1, rs2, xo, xi, xres, ag,
                 rq, pq, sq, tq, rg, pg, sg, tg, rd, pd, sd, td, ro, po, so, to,
                 sh, rt, sf, rh, sa, ra, r_y, s_y, r_x, s_x, r_gain, s_gain, lsem, dsem, osem):
    seq, dm, rows, qw, hd, ff, qc, kc = dims
    nk = qc // kc
    hs, qs = seq // 2, seq // 4
    n_dev = lax.axis_size("fsdp")
    n_chips = n_dev // 2
    me = lax.axis_index("fsdp")
    t = lax.axis_index("tp")
    chip, core = me // 2, me % 2
    other = 1 - core

    def dev(r, c):
        return 2 * lax.rem(chip + r, n_chips) + c

    right, left, partner, opposite = dev(RIGHT, core), dev(LEFT, core), dev(OWN, other), dev(OPP, core)

    def al(start, size):
        return pl.ds(pl.multiple_of(start, size), size)

    def remote(src, dst, ssem, rsem, target):
        return pltpu.make_async_remote_copy(src_ref=src, dst_ref=dst, send_sem=ssem, recv_sem=rsem,
                                            device_id=target, device_id_type=MESH)

    def send(src, dst, ssem, rsem, f):
        remote(src, dst, ssem, rsem, {"fsdp": f}).start()

    def wait_recv(ref, sem):
        remote(ref, ref, sem, sem, {"fsdp": partner}).wait_recv()

    def wait_send(ref, sem):
        remote(ref, ref, sem, sem, {"fsdp": partner}).wait_send()

    b0, b1 = t % 2, t // 2

    def y_plan(cc):
        if cc == 0:
            return t ^ 1, t ^ 3, (b0 + b1) % 2, b1
        return t ^ 3, t ^ 1, b1, b0

    def my_rows(cc):
        _, _, k1, k2 = y_plan(cc)
        return al(k1 * hs + k2 * qs, qs)

    barrier = pltpu.get_barrier_semaphore()
    for d in range(1, 8):
        pl.semaphore_signal(barrier, inc=1, device_id={"fsdp": lax.rem(me + d, n_dev)}, device_id_type=MESH)
    for m in (1, 3):
        pl.semaphore_signal(barrier, inc=1, device_id={"tp": t ^ m}, device_id_type=MESH)
    for f in range(dm // rows):
        pltpu.make_async_copy(x.at[:, pl.ds(f * rows, rows)], ag.at[f], osem.at[0]).start()
    pltpu.make_async_copy(pos, posv, osem.at[1]).start()
    pltpu.make_async_copy(freq, freqv, osem.at[2]).start()
    pltpu.make_async_copy(gain, gl.at[me], osem.at[3]).start()
    pl.semaphore_wait(barrier, 9)

    class Ring:
        def __init__(self, region, own, r, p, s, tp_):
            self.region, self.own, self.r, self.p, self.s, self.t = region, own, r, p, s, tp_

        def own_send(self, ab):
            for way, target, who in ((0, right, LEFT), (1, left, RIGHT)):
                for src, dst in self.own(ab):
                    send(src, dst, self.s.at[way, ab], self.r.at[who - 1, ab], target)
            for src, dst in self.own(ab):
                send(src, dst, self.t.at[OWN, ab], self.p.at[OWN, ab], partner)

        def pass_on(self, r, ab):
            ref = self.region(dev(r, core), ab)
            wait_recv(ref, self.r.at[r - 1, ab])
            send(ref, ref, self.t.at[r, ab], self.p.at[r, ab], partner)

        def service(self):
            for r, ab, target, way in ((LEFT, A, right, 0), (RIGHT, B, left, 1)):
                ref = self.region(dev(r, core), ab)
                wait_recv(ref, self.r.at[r - 1, ab])
                send(ref, ref, self.s.at[way, 2], self.r.at[OPP - 1, ab], target)
                send(ref, ref, self.t.at[r, ab], self.p.at[r, ab], partner)
            self.pass_on(LEFT, B)
            self.pass_on(RIGHT, A)

        def last(self):
            self.pass_on(OPP, A)
            self.pass_on(OPP, B)

        def wait_partner(self, r, ab):
            ref = self.region(dev(r, other), ab)
            wait_recv(ref, self.p.at[r, ab])
            return ref

        def drain(self):
            ref = self.region(0, A)
            for j in range(3):
                for way in (0, 1):
                    wait_send(ref, self.s.at[way, j])
            for r in range(4):
                for ab in (A, B):
                    wait_send(ref, self.t.at[r, ab])

    class Pair:
        def __init__(self, region, own, r, p, s, tp_):
            self.region, self.own, self.r, self.p, self.s, self.t = region, own, r, p, s, tp_

        def one(self, q, side, target, ssem, rsem):
            for src, dst in self.own(lax.rem(chip + q, n_chips), side):
                send(src, dst, ssem, rsem, target)

        def own_first(self):
            self.one(1, 0, right, self.s.at[0, 0], self.r.at[LEFT - 1, 0])
            self.one(2, 1, left, self.s.at[1, 0], self.r.at[RIGHT - 1, 1])

        def own_second(self):
            self.one(0, 1, right, self.s.at[0, 1], self.r.at[LEFT - 1, 1])
            self.one(3, 0, left, self.s.at[1, 1], self.r.at[RIGHT - 1, 0])
            self.one(0, 0, partner, self.t.at[OWN, 0], self.p.at[OWN, 0])
            self.one(3, 1, partner, self.t.at[OWN, 1], self.p.at[OWN, 1])

        def pass_on(self, r, side):
            ref = self.region(dev(r, core), side)
            wait_recv(ref, self.r.at[r - 1, side])
            send(ref, ref, self.t.at[r, side], self.p.at[r, side], partner)

        def forward(self):
            for r, side, target, way in ((LEFT, 0, right, 0), (RIGHT, 1, left, 1)):
                f = dev(r, core)
                ref = self.region(f, side)
                wait_recv(ref, self.r.at[r - 1, side])
                send(ref, self.region(f, 1 - side), self.s.at[way, 2], self.r.at[OPP - 1, 1 - side], target)
                send(ref, ref, self.t.at[r, side], self.p.at[r, side], partner)

        def rest(self):
            self.pass_on(LEFT, 1)
            self.pass_on(RIGHT, 0)

        def last(self):
            self.pass_on(OPP, 0)
            self.pass_on(OPP, 1)

        def wait_partner(self, r, side):
            ref = self.region(dev(r, other), side)
            wait_recv(ref, self.p.at[r, side])
            return ref

        def drain(self):
            ref = self.region(0, 0)
            for j in range(3):
                for way in (0, 1):
                    wait_send(ref, self.s.at[way, j])
            for r in range(4):
                for side in (0, 1):
                    wait_send(ref, self.t.at[r, side])

    def qkv_own(ab):
        if ab == A:
            return ((wq, lq.at[me, A]),)
        return ((wk, lq.at[me, B, :, pl.ds(0, hd)]), (wv, lq.at[me, B, :, pl.ds(hd, hd)]))

    qkv = Ring(lambda f, ab: lq.at[f, ab], qkv_own, rq, pq, sq, tq)

    def o_own(ab):
        return ((wo.at[pl.ds(ab * (qw // 2), qw // 2), :], lo.at[me, ab]),)

    w_o = Ring(lambda f, ab: lo.at[f, ab], o_own, ro, po, so, to)

    def gu(k):
        def own(q, side):
            cols = al(q * qc + k * kc, kc)
            return ((wg.at[:, cols], lg.at[k, side, me, A]), (wu.at[:, cols], lg.at[k, side, me, B]))

        return Pair(lambda f, side: lg.at[k, side, f], own, rg.at[k], pg.at[k], sg.at[k], tg.at[k])

    def d_own(q, side):
        return ((wd.at[al(q * qc, qc), :], ld.at[me, side]),)

    w_d = Pair(lambda f, side: ld.at[f, side], d_own, rd, pd, sd, td)

    def local(src, dst, sem):
        pltpu.make_async_copy(src, dst, sem).start()

    def finish_qkv():
        qkv.last()
        for src, cols, ab, off, width in ((wq, None, A, 0, qw), (wk, None, B, 0, hd), (wv, None, B, hd, hd)):
            local(src, stg.at[ab, me, :, pl.ds(off, width)], lsem)
        for ab in (A, B):
            for r in (RIGHT, LEFT, OPP):
                f = dev(r, core)
                local(lq.at[f, ab], stg.at[ab, f], lsem)
            for r in (OWN, RIGHT, LEFT, OPP):
                local(qkv.wait_partner(r, ab), stg.at[ab, dev(r, other)], lsem)
        pltpu.make_async_copy(stg, stg, lsem).wait()

    def finish_gu(k):
        flow = gu(k)

        def stage(r, mine):
            f = dev(r, core if mine else other)
            for side in (0, 1):
                cols = pl.ds(side * kc, kc)
                if not mine:
                    flow.wait_partner(r, side)
                for ab in (A, B):
                    local(lg.at[k, side, f, ab], stg.at[ab, f, :, cols], lsem)

        for side in (0, 1):
            q = lax.rem(chip + 3 * side, n_chips)
            for ab, src in ((A, wg), (B, wu)):
                local(src.at[:, al(q * qc + k * kc, kc)], stg.at[ab, me, :, pl.ds(side * kc, kc)], lsem)
        stage(RIGHT, True)
        stage(LEFT, True)
        stage(OWN, False)
        flow.last()
        stage(OPP, True)
        for r in (RIGHT, LEFT, OPP):
            stage(r, False)
        pltpu.make_async_copy(stg, stg, lsem).wait()

    hc = dm // 2

    def h_cols(cc):
        return pl.ds(cc * hc, hc)

    def rows_out():
        for cc, target in ((0, right), (1, left)):
            send(h.at[my_rows(cc), h_cols(cc)], tr.at[cc], sh.at[cc], rt.at[cc], target)

    def rows_forward():
        for cc, target in ((0, right), (1, left)):
            wait_recv(tr.at[cc], rt.at[cc])
            send(tr.at[cc], h2.at[my_rows(cc), h_cols(cc)], sf.at[cc], rh.at[cc], target)

    def rows_share(step):
        for cc in (0, 1):
            p1, p2, k1, k2 = y_plan(cc)
            if step == 0:
                mine = h2.at[my_rows(cc), h_cols(cc)]
                wait_recv(mine, rh.at[cc])
                remote(mine, mine, sa.at[cc, 0], ra.at[cc, 0], {"tp": p2}).start()
            elif step == 1:
                wait_recv(h2.at[al(k1 * hs + (1 - k2) * qs, qs), h_cols(cc)], ra.at[cc, 0])
                mine = h2.at[al(k1 * hs, hs), h_cols(cc)]
                remote(mine, mine, sa.at[cc, 1], ra.at[cc, 1], {"tp": p1}).start()
            else:
                wait_recv(h2.at[al((1 - k1) * hs, hs), h_cols(cc)], ra.at[cc, 1])

    def norm_tile(i, _):
        rr = al(i * 128, 128)
        blocks = [ag[f, rr, :].astype(jnp.float32) for f in range(dm // rows)]
        mean = sum(jnp.sum(b, axis=-1, keepdims=True) for b in blocks) * (1.0 / dm)
        cent = [b - mean for b in blocks]
        var = sum(jnp.sum(c * c, axis=-1, keepdims=True) for c in cent) * (1.0 / dm)
        scale = lax.rsqrt(var + NORM_EPS)
        for f in range(dm // rows):
            h[rr, f * rows:(f + 1) * rows] = (cent[f] * scale * gl[f]).astype(jnp.bfloat16)
        return _

    def rope_tile(i, _):
        angle = freqv[...] * posv[:, al(i * 128, 128)].astype(jnp.float32)
        cosv[al(i * 128, 128), :] = jnp.transpose(jnp.cos(angle))
        sinv[al(i * 128, 128), :] = jnp.transpose(jnp.sin(angle))
        return _

    def qkv_tile(i, _):
        rr = al(i * MT, MT)
        hm = h[rr, :]
        cs, sn = cosv[rr, :], sinv[rr, :]
        q = dot(hm, stg[A].reshape(dm, qw)).astype(jnp.bfloat16).astype(jnp.float32)
        kv = dot(hm, stg[B].reshape(dm, qw)).astype(jnp.bfloat16)
        for vec, base in ((q[:, :hd], 0), (q[:, hd:], hd), (kv[:, :hd].astype(jnp.float32), 2 * hd)):
            a, b = vec[:, :hd // 2], vec[:, hd // 2:]
            act[rr, base:base + hd // 2] = (a * cs - b * sn).astype(jnp.bfloat16)
            act[rr, base + hd // 2:base + hd] = (b * cs + a * sn).astype(jnp.bfloat16)
        act[rr, 3 * hd:] = kv[:, hd:]
        return _

    def attention(head):
        qb = 256

        def block(i, _):
            rr = al(i * qb, qb)
            s = lax.dot_general(act[rr, head * hd:(head + 1) * hd], act[:, 2 * hd:3 * hd],
                                (((1,), (1,)), ((), ())), preferred_element_type=jnp.float32) * (hd ** -0.5)
            qi = i * qb + lax.broadcasted_iota(jnp.int32, (qb, seq), 0)
            ki = lax.broadcasted_iota(jnp.int32, (qb, seq), 1)
            s = jnp.where(ki <= qi, s, -1e30)
            e = jnp.exp(s - jnp.max(s, axis=-1, keepdims=True))
            p = (e * (1.0 / jnp.sum(e, axis=-1, keepdims=True))).astype(jnp.bfloat16)
            o = dot(p, act[:, 3 * hd:])
            z[rr, 2 * qc + head * hd:2 * qc + (head + 1) * hd] = o.astype(jnp.bfloat16)
            return _

        lax.fori_loop(0, seq // qb, block, 0)

    def gate_up(k, src, dst):
        def tile(i, _):
            rr = al(i * MT, MT)
            hm = src[rr, :]
            g = dot(hm, stg[A].reshape(dm, 2 * kc)).astype(jnp.bfloat16).astype(jnp.float32)
            u = dot(hm, stg[B].reshape(dm, 2 * kc)).astype(jnp.bfloat16).astype(jnp.float32)
            r = (g * jax.nn.sigmoid(g) * u).astype(jnp.bfloat16)
            for side in (0, 1):
                dst[rr, side * qc + k * kc:side * qc + (k + 1) * kc] = r[:, side * kc:(side + 1) * kc]
            return _

        lax.fori_loop(0, seq // MT, tile, 0)

    def unit_f(g, cc):
        return dev(g, core if cc == 0 else other)

    def group_load(g):
        slot = SLOT[g]
        for cc in (0, 1):
            f = unit_f(g, cc)
            cols = pl.ds(cc * rows, rows)
            for side in (0, 1):
                dst = dstg.at[slot, pl.ds(side * qc, qc), cols]
                if g == OWN and cc == 0:
                    local(wd.at[al(lax.rem(chip + 3 * side, n_chips) * qc, qc), :], dst, dsem.at[slot])
                else:
                    if cc == 1:
                        w_d.wait_partner(g, side)
                    local(ld.at[f, side], dst, dsem.at[slot])

    def group_load_o(g):
        slot = SLOT[g]
        for cc in (0, 1):
            f = unit_f(g, cc)
            for ab in (A, B):
                dst = dstg.at[slot, pl.ds(2 * qc + ab * (qw // 2), qw // 2), pl.ds(cc * rows, rows)]
                if g == OWN and cc == 0:
                    local(wo.at[pl.ds(ab * (qw // 2), qw // 2), :], dst, dsem.at[2 + slot])
                else:
                    if cc == 1:
                        w_o.wait_partner(g, ab)
                    local(lo.at[f, ab], dst, dsem.at[2 + slot])

    def group_wait(g, s):
        slot = SLOT[g]
        ref = dstg.at[slot, pl.ds(0, 2 * qc), :] if s else dstg.at[slot, pl.ds(2 * qc, qw), :]
        pltpu.make_async_copy(ref, ref, dsem.at[2 * (1 - s) + slot]).wait()

    def group_part(g, s):
        group_wait(g, s)
        slot = SLOT[g]
        src, depth = ((z, 2 * qc + qw), (z2, 2 * qc))[s]

        def tile(i, _):
            rr = al(i * MT, MT)
            r = dot(src[rr, :], dstg[slot, :depth, :]).astype(jnp.bfloat16)
            for cc in (0, 1):
                part[slot, cc, s, rr, :] = r[:, cc * rows:(cc + 1) * rows]
            return _

        lax.fori_loop(0, seq // MT, tile, 0)
        for cc in (0, 1):
            p1, _, k1, _ = y_plan(cc)
            u = 2 * g + cc
            remote(part.at[slot, cc, s, al((1 - k1) * hs, hs), :], rs1.at[u, s],
                   s_y.at[u, 4 * s], r_y.at[u, 4 * s], {"tp": p1}).start()

    def sum_half(g):
        for cc in (0, 1):
            _, p2, k1, k2 = y_plan(cc)
            u = 2 * g + cc
            wait_recv(rs1.at[u, 1], r_y.at[u, 4])
            wait_recv(rs1.at[u, 0], r_y.at[u, 0])
            s1[u] = (part[SLOT[g], cc, :, al(k1 * hs, hs), :].astype(jnp.float32) + rs1[u].astype(jnp.float32)).astype(jnp.bfloat16)
            remote(s1.at[u, :, al((1 - k2) * qs, qs), :], rs2.at[u], s_y.at[u, 1], r_y.at[u, 1], {"tp": p2}).start()

    def part_free(g):
        for cc in (0, 1):
            for st in (0, 4):
                wait_send(rs1.at[0, 0], s_y.at[2 * g + cc, st])

    def sum_quarter(g):
        for cc in (0, 1):
            _, _, _, k2 = y_plan(cc)
            u = 2 * g + cc
            wait_recv(rs2.at[u], r_y.at[u, 1])
            mine = al(k2 * qs, qs)
            xo[u] = (s1[u, 1, mine, :].astype(jnp.float32) + rs2[u, 1].astype(jnp.float32)).astype(jnp.bfloat16)
            f = unit_f(g, cc)
            send(xo.at[u], xi.at[f], s_x.at[u], r_x.at[f], opposite)

    def close(g):
        for cc in (0, 1):
            _, p2, _, k2 = y_plan(cc)
            u = 2 * g + cc
            f = unit_f(g, cc)
            wait_recv(xi.at[f], r_x.at[f])
            mine = al(k2 * qs, qs)
            tot = s1[u, 0, mine, :].astype(jnp.float32) + rs2[u, 0].astype(jnp.float32) + xi[f].astype(jnp.float32)
            ag[u, my_rows(cc), :] = (xres[u].astype(jnp.float32) + tot).astype(jnp.bfloat16)
            ref = ag.at[u, my_rows(cc), :]
            remote(ref, ref, s_y.at[u, 2], r_y.at[u, 2], {"tp": p2}).start()

    def share_half(g):
        for cc in (0, 1):
            p1, _, k1, k2 = y_plan(cc)
            u = 2 * g + cc
            wait_recv(ag.at[u, al(k1 * hs + (1 - k2) * qs, qs), :], r_y.at[u, 2])
            ref = ag.at[u, al(k1 * hs, hs), :]
            remote(ref, ref, s_y.at[u, 3], r_y.at[u, 3], {"tp": p1}).start()

    def store(g):
        for cc in (0, 1):
            _, _, k1, _ = y_plan(cc)
            u = 2 * g + cc
            wait_recv(ag.at[u, al((1 - k1) * hs, hs), :], r_y.at[u, 3])
            local(ag.at[u], out.at[:, al(unit_f(g, cc) * rows, rows)], osem.at[4])

    for d in range(1, 8):
        f = lax.rem(me + d, n_dev)
        send(gain, gl.at[me], s_gain.at[d - 1], r_gain.at[d - 1], f)
    qkv.own_send(A)
    pltpu.make_async_copy(ag, ag, osem.at[0]).wait()
    pltpu.make_async_copy(gain, gl.at[me], osem.at[3]).wait()
    for d in range(1, 8):
        wait_recv(gl.at[lax.rem(me + n_dev - d, n_dev)], r_gain.at[d - 1])
    lax.fori_loop(0, seq // 128, norm_tile, 0)
    rows_out()
    qkv.own_send(B)
    pltpu.make_async_copy(pos, posv, osem.at[1]).wait()
    pltpu.make_async_copy(freq, freqv, osem.at[2]).wait()
    lax.fori_loop(0, seq // 128, rope_tile, 0)
    rows_forward()
    qkv.service()
    gu(0).own_first()
    gu(0).own_second()
    gu(1).own_first()
    rows_share(0)
    finish_qkv()
    lax.fori_loop(0, seq // MT, qkv_tile, 0)
    rows_share(1)
    attention(0)
    gu(0).forward()
    gu(1).own_second()
    gu(2).own_first()
    gu(0).rest()
    attention(1)
    finish_gu(0)
    gate_up(0, h, z)
    gu(1).forward()
    gu(2).own_second()
    gu(3).own_first()
    gu(1).rest()
    rows_share(2)
    gate_up(0, h2, z2)
    finish_gu(1)
    gu(2).forward()
    gu(3).own_second()
    gate_up(1, h, z)
    gu(2).rest()
    gate_up(1, h2, z2)
    gu(3).forward()
    w_d.own_first()
    w_d.own_second()
    w_o.own_send(A)
    w_o.own_send(B)
    finish_gu(2)
    gate_up(2, h, z)
    gu(3).rest()
    gate_up(2, h2, z2)
    group_load(OWN)
    group_load_o(OWN)
    for g in range(4):
        for cc in (0, 1):
            local(x.at[my_rows(cc), al(unit_f(g, cc) * rows, rows)], xres.at[2 * g + cc], osem.at[0])
    finish_gu(3)
    gate_up(3, h2, z2)
    group_part(OWN, 1)
    w_d.forward()
    gate_up(3, h, z)
    group_part(OWN, 0)
    w_d.rest()
    group_load(RIGHT)
    group_load(LEFT)
    group_part(RIGHT, 1)
    w_o.service()
    group_load_o(RIGHT)
    group_load_o(LEFT)
    group_part(RIGHT, 0)
    sum_half(OWN)
    part_free(OWN)
    group_part(LEFT, 1)
    group_part(LEFT, 0)
    w_d.last()
    w_o.last()
    group_load(OPP)
    group_load_o(OPP)
    sum_half(RIGHT)
    sum_quarter(OWN)
    sum_half(LEFT)
    part_free(RIGHT)
    group_part(OPP, 1)
    group_part(OPP, 0)
    pltpu.make_async_copy(xres, xres, osem.at[0]).wait()
    sum_quarter(RIGHT)
    sum_quarter(LEFT)
    close(LEFT)
    close(RIGHT)
    sum_half(OPP)
    share_half(LEFT)
    share_half(RIGHT)
    sum_quarter(OPP)
    close(OPP)
    close(OWN)
    store(LEFT)
    store(RIGHT)
    share_half(OPP)
    share_half(OWN)
    store(OPP)
    store(OWN)

    for d in range(1, 8):
        wait_send(gl.at[0], s_gain.at[d - 1])
    for cc in (0, 1):
        wait_send(tr.at[cc], sh.at[cc])
        wait_send(tr.at[cc], sf.at[cc])
        wait_send(h2.at[pl.ds(0, qs), h_cols(0)], sa.at[cc, 0])
        wait_send(h2.at[pl.ds(0, hs), h_cols(0)], sa.at[cc, 1])
    qkv.drain()
    w_o.drain()
    w_d.drain()
    for k in range(nk):
        gu(k).drain()
    for u in range(8):
        if u // 2 in (LEFT, OPP):
            wait_send(rs1.at[u, 0], s_y.at[u, 0])
            wait_send(rs1.at[u, 1], s_y.at[u, 4])
        wait_send(rs2.at[u], s_y.at[u, 1])
        wait_send(xo.at[u], s_x.at[u])
        wait_send(ag.at[u, pl.ds(0, qs), :], s_y.at[u, 2])
        wait_send(ag.at[u, pl.ds(0, hs), :], s_y.at[u, 3])
    pltpu.make_async_copy(ag, ag, osem.at[4]).wait()


def solution(mesh):
    row_spec = P(("dp", "fsdp"), None, None)

    def local_layer(hidden, positions, norm_gain, w_query, w_key, w_value, w_gate, w_up, w_out, w_down):
        _, seq, dm = hidden.shape
        rows, qw = w_query.shape
        hd = w_key.shape[1]
        ff = w_gate.shape[1]
        n_dev = dm // rows
        qc = ff // (n_dev // 2)
        kc = qw // 2
        nk = qc // kc
        inv_freq = 10000.0 ** (-jnp.arange(0, hd, 2, dtype=jnp.float32) / hd)
        bf, f32 = jnp.bfloat16, jnp.float32
        dma = pltpu.SemaphoreType.DMA
        dims = (seq, dm, rows, qw, hd, ff, qc, kc)
        anyspec = pl.BlockSpec(memory_space=pl.ANY)
        out = pl.pallas_call(
            functools.partial(layer_kernel, dims),
            out_shape=(jax.ShapeDtypeStruct((seq, dm), bf),
                       jax.ShapeDtypeStruct((n_dev, 2, rows, qw), bf),
                       jax.ShapeDtypeStruct((nk, 2, n_dev, 2, rows, kc), bf),
                       jax.ShapeDtypeStruct((n_dev, 2, qc, rows), bf),
                       jax.ShapeDtypeStruct((n_dev, 2, qw // 2, rows), bf)),
            in_specs=[anyspec] * 11,
            out_specs=(anyspec,) * 5,
            scratch_shapes=[
                pltpu.VMEM((seq, dm), bf),
                pltpu.VMEM((seq, dm), bf),
                pltpu.VMEM((seq, 2 * qc + qw), bf),
                pltpu.VMEM((seq, 2 * qc), bf),
                pltpu.VMEM((2, n_dev, rows, qw), bf),
                pltpu.VMEM((seq, 4 * hd), bf),
                pltpu.VMEM((1, seq), jnp.int32),
                pltpu.VMEM((hd // 2, 1), f32),
                pltpu.VMEM((seq, hd // 2), f32),
                pltpu.VMEM((seq, hd // 2), f32),
                pltpu.VMEM((n_dev, 1, rows), f32),
                pltpu.VMEM((2, seq // 4, dm // 2), bf),
                pltpu.VMEM((2, 2 * qc + qw, 2 * rows), bf),
                pltpu.VMEM((2, 2, 2, seq, rows), bf),
                pltpu.VMEM((8, 2, seq // 2, rows), bf),
                pltpu.VMEM((8, 2, seq // 2, rows), bf),
                pltpu.VMEM((8, 2, seq // 4, rows), bf),
                pltpu.VMEM((8, seq // 4, rows), bf),
                pltpu.VMEM((8, seq // 4, rows), bf),
                pltpu.VMEM((8, seq // 4, rows), bf),
                pltpu.VMEM((8, seq, rows), bf),
                dma((3, 2)), dma((4, 2)), dma((2, 3)), dma((4, 2)),
                dma((nk, 3, 2)), dma((nk, 4, 2)), dma((nk, 2, 3)), dma((nk, 4, 2)),
                dma((3, 2)), dma((4, 2)), dma((2, 3)), dma((4, 2)),
                dma((3, 2)), dma((4, 2)), dma((2, 3)), dma((4, 2)),
                dma((2,)), dma((2,)), dma((2,)), dma((2,)), dma((2, 2)), dma((2, 2)),
                dma((8, 5)), dma((8, 5)), dma((8,)), dma((8,)), dma((7,)), dma((7,)),
                dma, dma((4,)), dma((5,)),
            ],
            compiler_params=pltpu.CompilerParams(collective_id=0, has_side_effects=True,
                                                 vmem_limit_bytes=67043328),
        )(hidden.reshape(seq, dm), norm_gain.reshape(1, rows), positions.reshape(1, seq), inv_freq.reshape(hd // 2, 1),
          w_query, w_key, w_value, w_gate, w_up, w_out, w_down)[0]
        return out.reshape(hidden.shape)

    in_specs = (row_spec, P(None), P("fsdp"), P("fsdp", "tp"), P("fsdp", None), P("fsdp", None), P("fsdp", "tp"), P("fsdp", "tp"), P("tp", "fsdp"), P("tp", "fsdp"))
    return jax.shard_map(local_layer, mesh=mesh, in_specs=in_specs, out_specs=row_spec, check_vma=False)
```

```python
import functools

import jax
import jax.numpy as jnp
from jax import lax
from jax.experimental import pallas as pl
from jax.experimental.pallas import tpu as pltpu
from jax.sharding import PartitionSpec as P

NORM_EPS = 1e-6
MESH = pl.DeviceIdType.MESH
A, B = 0, 1
OWN, RIGHT, OPP, LEFT = 0, 1, 2, 3
MT = 512
SLOT = {OWN: 0, RIGHT: 1, LEFT: 0, OPP: 1}


def dot(a, b):
    return jnp.dot(a, b, preferred_element_type=jnp.float32)


def layer_kernel(dims, x, gain, pos, freq, wq, wk, wv, wg, wu, wo, wd,
                 out, lq, lg, ld, lo,
                 h, h2, z, z2, stg, act, posv, freqv, cosv, sinv, gl, tr, dstg, part, rs1, s1, rs2, xo, xi, xres, ag,
                 rq, pq, sq, tq, rkv, pkv, skv, tkv, rka, ska, rg, pg, sg, tg, rd, pd, sd, td, ro, po, so, to,
                 sh, rt, sf, rh, sa, ra, r_y, s_y, r_x, s_x, r_gain, s_gain, lsem, dsem, osem):
    seq, dm, rows, qw, hd, ff, qc, kc = dims
    nk = qc // kc
    hs, qs = seq // 2, seq // 4
    n_dev = lax.axis_size("fsdp")
    n_chips = n_dev // 2
    me = lax.axis_index("fsdp")
    t = lax.axis_index("tp")
    chip, core = me // 2, me % 2
    other = 1 - core

    def dev(r, c):
        return 2 * lax.rem(chip + r, n_chips) + c

    right, left, partner, opposite = dev(RIGHT, core), dev(LEFT, core), dev(OWN, other), dev(OPP, core)

    def al(start, size):
        return pl.ds(pl.multiple_of(start, size), size)

    def remote(src, dst, ssem, rsem, target):
        return pltpu.make_async_remote_copy(src_ref=src, dst_ref=dst, send_sem=ssem, recv_sem=rsem,
                                            device_id=target, device_id_type=MESH)

    def send(src, dst, ssem, rsem, f):
        remote(src, dst, ssem, rsem, {"fsdp": f}).start()

    def wait_recv(ref, sem):
        remote(ref, ref, sem, sem, {"fsdp": partner}).wait_recv()

    def wait_send(ref, sem):
        remote(ref, ref, sem, sem, {"fsdp": partner}).wait_send()

    b0, b1 = t % 2, t // 2

    def y_plan(cc):
        if cc == 0:
            return t ^ 1, t ^ 3, (b0 + b1) % 2, b1
        return t ^ 3, t ^ 1, b1, b0

    def my_rows(cc):
        _, _, k1, k2 = y_plan(cc)
        return al(k1 * hs + k2 * qs, qs)

    barrier = pltpu.get_barrier_semaphore()
    for d in range(1, 8):
        pl.semaphore_signal(barrier, inc=1, device_id={"fsdp": lax.rem(me + d, n_dev)}, device_id_type=MESH)
    for m in (1, 3):
        pl.semaphore_signal(barrier, inc=1, device_id={"tp": t ^ m}, device_id_type=MESH)
    for f in range(dm // rows):
        pltpu.make_async_copy(x.at[:, pl.ds(f * rows, rows)], ag.at[f], osem.at[0]).start()
    pltpu.make_async_copy(pos, posv, osem.at[1]).start()
    pltpu.make_async_copy(freq, freqv, osem.at[2]).start()
    pltpu.make_async_copy(gain, gl.at[me], osem.at[3]).start()
    pl.semaphore_wait(barrier, 9)

    class Ring:
        def __init__(self, region, own, r, p, s, tp_):
            self.region, self.own, self.r, self.p, self.s, self.t = region, own, r, p, s, tp_

        def own_send(self, ab):
            for way, target, who in ((0, right, LEFT), (1, left, RIGHT)):
                for src, dst in self.own(ab):
                    send(src, dst, self.s.at[way, ab], self.r.at[who - 1, ab], target)
            for src, dst in self.own(ab):
                send(src, dst, self.t.at[OWN, ab], self.p.at[OWN, ab], partner)

        def pass_on(self, r, ab):
            ref = self.region(dev(r, core), ab)
            wait_recv(ref, self.r.at[r - 1, ab])
            send(ref, ref, self.t.at[r, ab], self.p.at[r, ab], partner)

        def service(self):
            for r, ab, target, way in ((LEFT, A, right, 0), (RIGHT, B, left, 1)):
                ref = self.region(dev(r, core), ab)
                wait_recv(ref, self.r.at[r - 1, ab])
                send(ref, ref, self.s.at[way, 2], self.r.at[OPP - 1, ab], target)
                send(ref, ref, self.t.at[r, ab], self.p.at[r, ab], partner)
            self.pass_on(LEFT, B)
            self.pass_on(RIGHT, A)

        def last(self):
            self.pass_on(OPP, A)
            self.pass_on(OPP, B)

        def wait_partner(self, r, ab):
            ref = self.region(dev(r, other), ab)
            wait_recv(ref, self.p.at[r, ab])
            return ref

        def drain(self):
            ref = self.region(0, A)
            for j in range(3):
                for way in (0, 1):
                    wait_send(ref, self.s.at[way, j])
            for r in range(4):
                for ab in (A, B):
                    wait_send(ref, self.t.at[r, ab])

    class Pair:
        def __init__(self, region, own, r, p, s, tp_):
            self.region, self.own, self.r, self.p, self.s, self.t = region, own, r, p, s, tp_

        def one(self, q, side, target, ssem, rsem):
            for src, dst in self.own(lax.rem(chip + q, n_chips), side):
                send(src, dst, ssem, rsem, target)

        def own_first(self):
            self.one(1, 0, right, self.s.at[0, 0], self.r.at[LEFT - 1, 0])
            self.one(2, 1, left, self.s.at[1, 0], self.r.at[RIGHT - 1, 1])

        def own_second(self):
            self.one(0, 1, right, self.s.at[0, 1], self.r.at[LEFT - 1, 1])
            self.one(3, 0, left, self.s.at[1, 1], self.r.at[RIGHT - 1, 0])
            self.one(0, 0, partner, self.t.at[OWN, 0], self.p.at[OWN, 0])
            self.one(3, 1, partner, self.t.at[OWN, 1], self.p.at[OWN, 1])

        def pass_on(self, r, side):
            ref = self.region(dev(r, core), side)
            wait_recv(ref, self.r.at[r - 1, side])
            send(ref, ref, self.t.at[r, side], self.p.at[r, side], partner)

        def forward(self):
            for r, side, target, way in ((LEFT, 0, right, 0), (RIGHT, 1, left, 1)):
                f = dev(r, core)
                ref = self.region(f, side)
                wait_recv(ref, self.r.at[r - 1, side])
                send(ref, self.region(f, 1 - side), self.s.at[way, 2], self.r.at[OPP - 1, 1 - side], target)
                send(ref, ref, self.t.at[r, side], self.p.at[r, side], partner)

        def rest(self):
            self.pass_on(LEFT, 1)
            self.pass_on(RIGHT, 0)

        def last(self):
            self.pass_on(OPP, 0)
            self.pass_on(OPP, 1)

        def wait_partner(self, r, side):
            ref = self.region(dev(r, other), side)
            wait_recv(ref, self.p.at[r, side])
            return ref

        def drain(self):
            ref = self.region(0, 0)
            for j in range(3):
                for way in (0, 1):
                    wait_send(ref, self.s.at[way, j])
            for r in range(4):
                for side in (0, 1):
                    wait_send(ref, self.t.at[r, side])

    half = rows // 2

    def q_region(f, ab):
        return lq.at[f, A, pl.ds(ab * half, half), :]

    qkv = Ring(q_region, lambda ab: ((wq.at[pl.ds(ab * half, half), :], q_region(me, ab)),), rq, pq, sq, tq)

    kv_cols = ((wk, pl.ds(0, hd)), (wv, pl.ds(hd, hd)))
    kv_p1, kv_p2 = t ^ (1 + 2 * core), t ^ (3 - 2 * core)
    kv_k1 = core * b1 + other * lax.rem(b0 + b1, 2)
    kv_k2 = core * b0 + other * b1
    kq = rows // 4
    kv_rows = al(kv_k1 * half + kv_k2 * kq, kq)

    def kv_send():
        for r, who in ((RIGHT, LEFT), (LEFT, RIGHT), (OPP, OPP)):
            for src, cols in kv_cols:
                send(src.at[kv_rows, :], lq.at[me, B, kv_rows, cols], skv.at[r - 1], rkv.at[who - 1], dev(r, core))
        for src, cols in kv_cols:
            send(src, lq.at[me, B, :, cols], tkv.at[OWN], pkv.at[OWN], partner)

    def kv_share(step):
        for r in (RIGHT, OPP, LEFT):
            f = dev(r, core)
            if step == 0:
                ref = lq.at[f, B, kv_rows, :]
                wait_recv(ref, rkv.at[r - 1])
                remote(ref, ref, ska.at[0, r - 1], rka.at[0, r - 1], {"tp": kv_p2}).start()
            elif step == 1:
                wait_recv(lq.at[f, B, al(kv_k1 * half + (1 - kv_k2) * kq, kq), :], rka.at[0, r - 1])
                ref = lq.at[f, B, al(kv_k1 * half, half), :]
                remote(ref, ref, ska.at[1, r - 1], rka.at[1, r - 1], {"tp": kv_p1}).start()
            else:
                wait_recv(lq.at[f, B, al((1 - kv_k1) * half, half), :], rka.at[1, r - 1])
                ref = lq.at[f, B]
                send(ref, ref, tkv.at[r], pkv.at[r], partner)

    def kv_drain():
        for r in range(3):
            wait_send(lq.at[0, B, pl.ds(0, kq), :], skv.at[r])
            wait_send(lq.at[0, B, pl.ds(0, kq), :], ska.at[0, r])
            wait_send(lq.at[0, B, pl.ds(0, half), :], ska.at[1, r])
        for r in range(4):
            wait_send(lq.at[0, B], tkv.at[r])

    def o_own(ab):
        return ((wo.at[pl.ds(ab * (qw // 2), qw // 2), :], lo.at[me, ab]),)

    w_o = Ring(lambda f, ab: lo.at[f, ab], o_own, ro, po, so, to)

    def gu(k):
        def own(q, side):
            cols = al(q * qc + k * kc, kc)
            return ((wg.at[:, cols], lg.at[k, side, me, A]), (wu.at[:, cols], lg.at[k, side, me, B]))

        return Pair(lambda f, side: lg.at[k, side, f], own, rg.at[k], pg.at[k], sg.at[k], tg.at[k])

    def d_own(q, side):
        return ((wd.at[al(q * qc, qc), :], ld.at[me, side]),)

    w_d = Pair(lambda f, side: ld.at[f, side], d_own, rd, pd, sd, td)

    def local(src, dst, sem):
        pltpu.make_async_copy(src, dst, sem).start()

    def finish_qkv():
        qkv.last()
        for src, ab, off, width in ((wq, A, 0, qw), (wk, B, 0, hd), (wv, B, hd, hd)):
            local(src, stg.at[ab, me, :, pl.ds(off, width)], lsem)
        for ab in (A, B):
            for r in (RIGHT, LEFT, OPP):
                f = dev(r, core)
                local(lq.at[f, ab], stg.at[ab, f], lsem)
        for r in (OWN, RIGHT, LEFT, OPP):
            f = dev(r, other)
            for ab in (A, B):
                qkv.wait_partner(r, ab)
            wait_recv(lq.at[f, B], pkv.at[r])
            for ab in (A, B):
                local(lq.at[f, ab], stg.at[ab, f], lsem)
        pltpu.make_async_copy(stg, stg, lsem).wait()

    def finish_gu(k):
        flow = gu(k)

        def stage(r, mine):
            f = dev(r, core if mine else other)
            for side in (0, 1):
                cols = pl.ds(side * kc, kc)
                if not mine:
                    flow.wait_partner(r, side)
                for ab in (A, B):
                    local(lg.at[k, side, f, ab], stg.at[ab, f, :, cols], lsem)

        for side in (0, 1):
            q = lax.rem(chip + 3 * side, n_chips)
            for ab, src in ((A, wg), (B, wu)):
                local(src.at[:, al(q * qc + k * kc, kc)], stg.at[ab, me, :, pl.ds(side * kc, kc)], lsem)
        stage(RIGHT, True)
        stage(LEFT, True)
        stage(OWN, False)
        flow.last()
        stage(OPP, True)
        for r in (RIGHT, LEFT, OPP):
            stage(r, False)
        pltpu.make_async_copy(stg, stg, lsem).wait()

    hc = dm // 2

    def h_cols(cc):
        return pl.ds(cc * hc, hc)

    def rows_out():
        for cc, target in ((0, right), (1, left)):
            send(h.at[my_rows(cc), h_cols(cc)], tr.at[cc], sh.at[cc], rt.at[cc], target)

    def rows_forward():
        for cc, target in ((0, right), (1, left)):
            wait_recv(tr.at[cc], rt.at[cc])
            send(tr.at[cc], h2.at[my_rows(cc), h_cols(cc)], sf.at[cc], rh.at[cc], target)

    def rows_share(step):
        for cc in (0, 1):
            p1, p2, k1, k2 = y_plan(cc)
            if step == 0:
                mine = h2.at[my_rows(cc), h_cols(cc)]
                wait_recv(mine, rh.at[cc])
                remote(mine, mine, sa.at[cc, 0], ra.at[cc, 0], {"tp": p2}).start()
            elif step == 1:
                wait_recv(h2.at[al(k1 * hs + (1 - k2) * qs, qs), h_cols(cc)], ra.at[cc, 0])
                mine = h2.at[al(k1 * hs, hs), h_cols(cc)]
                remote(mine, mine, sa.at[cc, 1], ra.at[cc, 1], {"tp": p1}).start()
            else:
                wait_recv(h2.at[al((1 - k1) * hs, hs), h_cols(cc)], ra.at[cc, 1])

    def norm_tile(i, _):
        rr = al(i * 128, 128)
        blocks = [ag[f, rr, :].astype(jnp.float32) for f in range(dm // rows)]
        mean = sum(jnp.sum(b, axis=-1, keepdims=True) for b in blocks) * (1.0 / dm)
        cent = [b - mean for b in blocks]
        var = sum(jnp.sum(c * c, axis=-1, keepdims=True) for c in cent) * (1.0 / dm)
        scale = lax.rsqrt(var + NORM_EPS)
        for f in range(dm // rows):
            h[rr, f * rows:(f + 1) * rows] = (cent[f] * scale * gl[f]).astype(jnp.bfloat16)
        return _

    def rope_tile(i, _):
        angle = freqv[...] * posv[:, al(i * 128, 128)].astype(jnp.float32)
        cosv[al(i * 128, 128), :] = jnp.transpose(jnp.cos(angle))
        sinv[al(i * 128, 128), :] = jnp.transpose(jnp.sin(angle))
        return _

    def qkv_tile(i, _):
        rr = al(i * MT, MT)
        hm = h[rr, :]
        cs, sn = cosv[rr, :], sinv[rr, :]
        q = dot(hm, stg[A].reshape(dm, qw)).astype(jnp.bfloat16).astype(jnp.float32)
        kv = dot(hm, stg[B].reshape(dm, qw)).astype(jnp.bfloat16)
        for vec, base in ((q[:, :hd], 0), (q[:, hd:], hd), (kv[:, :hd].astype(jnp.float32), 2 * hd)):
            a, b = vec[:, :hd // 2], vec[:, hd // 2:]
            act[rr, base:base + hd // 2] = (a * cs - b * sn).astype(jnp.bfloat16)
            act[rr, base + hd // 2:base + hd] = (b * cs + a * sn).astype(jnp.bfloat16)
        act[rr, 3 * hd:] = kv[:, hd:]
        return _

    def attention(head):
        qb = 256

        def block(i, _):
            rr = al(i * qb, qb)
            s = lax.dot_general(act[rr, head * hd:(head + 1) * hd], act[:, 2 * hd:3 * hd],
                                (((1,), (1,)), ((), ())), preferred_element_type=jnp.float32) * (hd ** -0.5)
            qi = i * qb + lax.broadcasted_iota(jnp.int32, (qb, seq), 0)
            ki = lax.broadcasted_iota(jnp.int32, (qb, seq), 1)
            s = jnp.where(ki <= qi, s, -1e30)
            e = jnp.exp(s - jnp.max(s, axis=-1, keepdims=True))
            p = (e * (1.0 / jnp.sum(e, axis=-1, keepdims=True))).astype(jnp.bfloat16)
            o = dot(p, act[:, 3 * hd:])
            z[rr, 2 * qc + head * hd:2 * qc + (head + 1) * hd] = o.astype(jnp.bfloat16)
            return _

        lax.fori_loop(0, seq // qb, block, 0)

    def gate_up(k, src, dst):
        def tile(i, _):
            rr = al(i * MT, MT)
            hm = src[rr, :]
            g = dot(hm, stg[A].reshape(dm, 2 * kc)).astype(jnp.bfloat16).astype(jnp.float32)
            u = dot(hm, stg[B].reshape(dm, 2 * kc)).astype(jnp.bfloat16).astype(jnp.float32)
            r = (g * jax.nn.sigmoid(g) * u).astype(jnp.bfloat16)
            for side in (0, 1):
                dst[rr, side * qc + k * kc:side * qc + (k + 1) * kc] = r[:, side * kc:(side + 1) * kc]
            return _

        lax.fori_loop(0, seq // MT, tile, 0)

    def unit_f(g, cc):
        return dev(g, core if cc == 0 else other)

    def group_load(g):
        slot = SLOT[g]
        for cc in (0, 1):
            f = unit_f(g, cc)
            cols = pl.ds(cc * rows, rows)
            for side in (0, 1):
                dst = dstg.at[slot, pl.ds(side * qc, qc), cols]
                if g == OWN and cc == 0:
                    local(wd.at[al(lax.rem(chip + 3 * side, n_chips) * qc, qc), :], dst, dsem.at[slot])
                else:
                    if cc == 1:
                        w_d.wait_partner(g, side)
                    local(ld.at[f, side], dst, dsem.at[slot])

    def group_load_o(g):
        slot = SLOT[g]
        for cc in (0, 1):
            f = unit_f(g, cc)
            for ab in (A, B):
                dst = dstg.at[slot, pl.ds(2 * qc + ab * (qw // 2), qw // 2), pl.ds(cc * rows, rows)]
                if g == OWN and cc == 0:
                    local(wo.at[pl.ds(ab * (qw // 2), qw // 2), :], dst, dsem.at[2 + slot])
                else:
                    if cc == 1:
                        w_o.wait_partner(g, ab)
                    local(lo.at[f, ab], dst, dsem.at[2 + slot])

    def group_wait(g, s):
        slot = SLOT[g]
        ref = dstg.at[slot, pl.ds(0, 2 * qc), :] if s else dstg.at[slot, pl.ds(2 * qc, qw), :]
        pltpu.make_async_copy(ref, ref, dsem.at[2 * (1 - s) + slot]).wait()

    def group_part(g, s):
        group_wait(g, s)
        slot = SLOT[g]
        src, depth = ((z, 2 * qc + qw), (z2, 2 * qc))[s]

        def tile(i, _):
            rr = al(i * MT, MT)
            r = dot(src[rr, :], dstg[slot, :depth, :]).astype(jnp.bfloat16)
            for cc in (0, 1):
                part[slot, cc, s, rr, :] = r[:, cc * rows:(cc + 1) * rows]
            return _

        lax.fori_loop(0, seq // MT, tile, 0)
        for cc in (0, 1):
            p1, _, k1, _ = y_plan(cc)
            u = 2 * g + cc
            remote(part.at[slot, cc, s, al((1 - k1) * hs, hs), :], rs1.at[u, s],
                   s_y.at[u, 4 * s], r_y.at[u, 4 * s], {"tp": p1}).start()

    def sum_half(g):
        for cc in (0, 1):
            _, p2, k1, k2 = y_plan(cc)
            u = 2 * g + cc
            wait_recv(rs1.at[u, 1], r_y.at[u, 4])
            wait_recv(rs1.at[u, 0], r_y.at[u, 0])
            s1[u] = (part[SLOT[g], cc, :, al(k1 * hs, hs), :].astype(jnp.float32) + rs1[u].astype(jnp.float32)).astype(jnp.bfloat16)
            remote(s1.at[u, :, al((1 - k2) * qs, qs), :], rs2.at[u], s_y.at[u, 1], r_y.at[u, 1], {"tp": p2}).start()

    def part_free(g):
        for cc in (0, 1):
            for st in (0, 4):
                wait_send(rs1.at[0, 0], s_y.at[2 * g + cc, st])

    def sum_quarter(g):
        for cc in (0, 1):
            _, _, _, k2 = y_plan(cc)
            u = 2 * g + cc
            wait_recv(rs2.at[u], r_y.at[u, 1])
            mine = al(k2 * qs, qs)
            xo[u] = (s1[u, 1, mine, :].astype(jnp.float32) + rs2[u, 1].astype(jnp.float32)).astype(jnp.bfloat16)
            f = unit_f(g, cc)
            send(xo.at[u], xi.at[f], s_x.at[u], r_x.at[f], opposite)

    def close(g):
        for cc in (0, 1):
            _, p2, _, k2 = y_plan(cc)
            u = 2 * g + cc
            f = unit_f(g, cc)
            wait_recv(xi.at[f], r_x.at[f])
            mine = al(k2 * qs, qs)
            tot = s1[u, 0, mine, :].astype(jnp.float32) + rs2[u, 0].astype(jnp.float32) + xi[f].astype(jnp.float32)
            ag[u, my_rows(cc), :] = (xres[u].astype(jnp.float32) + tot).astype(jnp.bfloat16)
            ref = ag.at[u, my_rows(cc), :]
            remote(ref, ref, s_y.at[u, 2], r_y.at[u, 2], {"tp": p2}).start()

    def share_half(g):
        for cc in (0, 1):
            p1, _, k1, k2 = y_plan(cc)
            u = 2 * g + cc
            wait_recv(ag.at[u, al(k1 * hs + (1 - k2) * qs, qs), :], r_y.at[u, 2])
            ref = ag.at[u, al(k1 * hs, hs), :]
            remote(ref, ref, s_y.at[u, 3], r_y.at[u, 3], {"tp": p1}).start()

    def store(g):
        for cc in (0, 1):
            _, _, k1, _ = y_plan(cc)
            u = 2 * g + cc
            wait_recv(ag.at[u, al((1 - k1) * hs, hs), :], r_y.at[u, 3])
            local(ag.at[u], out.at[:, al(unit_f(g, cc) * rows, rows)], osem.at[4])

    for d in range(1, 8):
        f = lax.rem(me + d, n_dev)
        send(gain, gl.at[me], s_gain.at[d - 1], r_gain.at[d - 1], f)
    qkv.own_send(A)
    qkv.own_send(B)
    kv_send()
    pltpu.make_async_copy(ag, ag, osem.at[0]).wait()
    pltpu.make_async_copy(gain, gl.at[me], osem.at[3]).wait()
    for d in range(1, 8):
        wait_recv(gl.at[lax.rem(me + n_dev - d, n_dev)], r_gain.at[d - 1])
    lax.fori_loop(0, seq // 128, norm_tile, 0)
    rows_out()
    qkv.service()
    kv_share(0)
    pltpu.make_async_copy(pos, posv, osem.at[1]).wait()
    pltpu.make_async_copy(freq, freqv, osem.at[2]).wait()
    lax.fori_loop(0, seq // 128, rope_tile, 0)
    kv_share(1)
    rows_forward()
    gu(0).own_first()
    gu(0).own_second()
    gu(1).own_first()
    kv_share(2)
    finish_qkv()
    lax.fori_loop(0, seq // MT, qkv_tile, 0)
    rows_share(0)
    attention(0)
    gu(0).forward()
    gu(1).own_second()
    gu(2).own_first()
    attention(1)
    gu(0).rest()
    rows_share(1)
    finish_gu(0)
    gu(1).forward()
    gu(2).own_second()
    gu(3).own_first()
    gate_up(0, h, z)
    gu(1).rest()
    rows_share(2)
    gu(2).forward()
    gu(3).own_second()
    gate_up(0, h2, z2)
    finish_gu(1)
    gate_up(1, h, z)
    gu(2).rest()
    gate_up(1, h2, z2)
    gu(3).forward()
    w_d.own_first()
    w_d.own_second()
    w_o.own_send(A)
    w_o.own_send(B)
    finish_gu(2)
    gate_up(2, h, z)
    gu(3).rest()
    gate_up(2, h2, z2)
    group_load(OWN)
    group_load_o(OWN)
    for g in range(4):
        for cc in (0, 1):
            local(x.at[my_rows(cc), al(unit_f(g, cc) * rows, rows)], xres.at[2 * g + cc], osem.at[0])
    finish_gu(3)
    gate_up(3, h2, z2)
    group_part(OWN, 1)
    w_d.forward()
    gate_up(3, h, z)
    group_part(OWN, 0)
    w_d.rest()
    group_load(RIGHT)
    group_load(LEFT)
    group_part(RIGHT, 1)
    w_o.service()
    group_load_o(RIGHT)
    group_load_o(LEFT)
    group_part(RIGHT, 0)
    sum_half(OWN)
    part_free(OWN)
    group_part(LEFT, 1)
    group_part(LEFT, 0)
    w_d.last()
    w_o.last()
    group_load(OPP)
    group_load_o(OPP)
    sum_half(RIGHT)
    sum_quarter(OWN)
    sum_half(LEFT)
    part_free(RIGHT)
    group_part(OPP, 1)
    group_part(OPP, 0)
    pltpu.make_async_copy(xres, xres, osem.at[0]).wait()
    sum_quarter(RIGHT)
    sum_quarter(LEFT)
    close(LEFT)
    close(RIGHT)
    sum_half(OPP)
    share_half(LEFT)
    share_half(RIGHT)
    sum_quarter(OPP)
    close(OPP)
    close(OWN)
    store(LEFT)
    store(RIGHT)
    share_half(OPP)
    share_half(OWN)
    store(OPP)
    store(OWN)

    for d in range(1, 8):
        wait_send(gl.at[0], s_gain.at[d - 1])
    for cc in (0, 1):
        wait_send(tr.at[cc], sh.at[cc])
        wait_send(tr.at[cc], sf.at[cc])
        wait_send(h2.at[pl.ds(0, qs), h_cols(0)], sa.at[cc, 0])
        wait_send(h2.at[pl.ds(0, hs), h_cols(0)], sa.at[cc, 1])
    qkv.drain()
    kv_drain()
    w_o.drain()
    w_d.drain()
    for k in range(nk):
        gu(k).drain()
    for u in range(8):
        if u // 2 in (LEFT, OPP):
            wait_send(rs1.at[u, 0], s_y.at[u, 0])
            wait_send(rs1.at[u, 1], s_y.at[u, 4])
        wait_send(rs2.at[u], s_y.at[u, 1])
        wait_send(xo.at[u], s_x.at[u])
        wait_send(ag.at[u, pl.ds(0, qs), :], s_y.at[u, 2])
        wait_send(ag.at[u, pl.ds(0, hs), :], s_y.at[u, 3])
    pltpu.make_async_copy(ag, ag, osem.at[4]).wait()


def solution(mesh):
    row_spec = P(("dp", "fsdp"), None, None)

    def local_layer(hidden, positions, norm_gain, w_query, w_key, w_value, w_gate, w_up, w_out, w_down):
        _, seq, dm = hidden.shape
        rows, qw = w_query.shape
        hd = w_key.shape[1]
        ff = w_gate.shape[1]
        n_dev = dm // rows
        qc = ff // (n_dev // 2)
        kc = qw // 2
        nk = qc // kc
        inv_freq = 10000.0 ** (-jnp.arange(0, hd, 2, dtype=jnp.float32) / hd)
        bf, f32 = jnp.bfloat16, jnp.float32
        dma = pltpu.SemaphoreType.DMA
        dims = (seq, dm, rows, qw, hd, ff, qc, kc)
        anyspec = pl.BlockSpec(memory_space=pl.ANY)
        out = pl.pallas_call(
            functools.partial(layer_kernel, dims),
            out_shape=(jax.ShapeDtypeStruct((seq, dm), bf),
                       jax.ShapeDtypeStruct((n_dev, 2, rows, qw), bf),
                       jax.ShapeDtypeStruct((nk, 2, n_dev, 2, rows, kc), bf),
                       jax.ShapeDtypeStruct((n_dev, 2, qc, rows), bf),
                       jax.ShapeDtypeStruct((n_dev, 2, qw // 2, rows), bf)),
            in_specs=[anyspec] * 11,
            out_specs=(anyspec,) * 5,
            scratch_shapes=[
                pltpu.VMEM((seq, dm), bf),
                pltpu.VMEM((seq, dm), bf),
                pltpu.VMEM((seq, 2 * qc + qw), bf),
                pltpu.VMEM((seq, 2 * qc), bf),
                pltpu.VMEM((2, n_dev, rows, qw), bf),
                pltpu.VMEM((seq, 4 * hd), bf),
                pltpu.VMEM((1, seq), jnp.int32),
                pltpu.VMEM((hd // 2, 1), f32),
                pltpu.VMEM((seq, hd // 2), f32),
                pltpu.VMEM((seq, hd // 2), f32),
                pltpu.VMEM((n_dev, 1, rows), f32),
                pltpu.VMEM((2, seq // 4, dm // 2), bf),
                pltpu.VMEM((2, 2 * qc + qw, 2 * rows), bf),
                pltpu.VMEM((2, 2, 2, seq, rows), bf),
                pltpu.VMEM((8, 2, seq // 2, rows), bf),
                pltpu.VMEM((8, 2, seq // 2, rows), bf),
                pltpu.VMEM((8, 2, seq // 4, rows), bf),
                pltpu.VMEM((8, seq // 4, rows), bf),
                pltpu.VMEM((8, seq // 4, rows), bf),
                pltpu.VMEM((8, seq // 4, rows), bf),
                pltpu.VMEM((8, seq, rows), bf),
                dma((3, 2)), dma((4, 2)), dma((2, 3)), dma((4, 2)),
                dma((3,)), dma((4,)), dma((3,)), dma((4,)), dma((2, 3)), dma((2, 3)),
                dma((nk, 3, 2)), dma((nk, 4, 2)), dma((nk, 2, 3)), dma((nk, 4, 2)),
                dma((3, 2)), dma((4, 2)), dma((2, 3)), dma((4, 2)),
                dma((3, 2)), dma((4, 2)), dma((2, 3)), dma((4, 2)),
                dma((2,)), dma((2,)), dma((2,)), dma((2,)), dma((2, 2)), dma((2, 2)),
                dma((8, 5)), dma((8, 5)), dma((8,)), dma((8,)), dma((7,)), dma((7,)),
                dma, dma((4,)), dma((5,)),
            ],
            compiler_params=pltpu.CompilerParams(collective_id=0, has_side_effects=True,
                                                 vmem_limit_bytes=67043328),
        )(hidden.reshape(seq, dm), norm_gain.reshape(1, rows), positions.reshape(1, seq), inv_freq.reshape(hd // 2, 1),
          w_query, w_key, w_value, w_gate, w_up, w_out, w_down)[0]
        return out.reshape(hidden.shape)

    in_specs = (row_spec, P(None), P("fsdp"), P("fsdp", "tp"), P("fsdp", None), P("fsdp", None), P("fsdp", "tp"), P("fsdp", "tp"), P("tp", "fsdp"), P("tp", "fsdp"))
    return jax.shard_map(local_layer, mesh=mesh, in_specs=in_specs, out_specs=row_spec, check_vma=False)
```

```python
import functools

import jax
import jax.numpy as jnp
from jax import lax
from jax.experimental import pallas as pl
from jax.experimental.pallas import tpu as pltpu
from jax.sharding import PartitionSpec as P

NORM_EPS = 1e-6
MESH = pl.DeviceIdType.MESH
A, B = 0, 1
OWN, RIGHT, OPP, LEFT = 0, 1, 2, 3
MT = 512
SLOT = {OWN: 0, RIGHT: 1, LEFT: 0, OPP: 1}


def dot(a, b):
    return jnp.dot(a, b, preferred_element_type=jnp.float32)


def layer_kernel(dims, x, gain, pos, freq, wq, wk, wv, wg, wu, wo, wd,
                 out, lq, lg, ld, lo,
                 h, h2, z, z2, stg, act, posv, freqv, cosv, sinv, gl, tr, dstg, part, rs1, s1, rs2, xo, xi, xres, ag,
                 rq, pq, sq, tq, rkv, pkv, skv, tkv, rka, ska, rg, pg, sg, tg, rd, pd, sd, td, ro, po, so, to,
                 sh, rt, sf, rh, sa, ra, r_y, s_y, r_x, s_x, r_gain, s_gain, lsem, dsem, osem):
    seq, dm, rows, qw, hd, ff, qc, kc = dims
    nk = qc // kc
    hs, qs = seq // 2, seq // 4
    n_dev = lax.axis_size("fsdp")
    n_chips = n_dev // 2
    me = lax.axis_index("fsdp")
    t = lax.axis_index("tp")
    chip, core = me // 2, me % 2
    other = 1 - core

    def dev(r, c):
        return 2 * lax.rem(chip + r, n_chips) + c

    right, left, partner, opposite = dev(RIGHT, core), dev(LEFT, core), dev(OWN, other), dev(OPP, core)

    def al(start, size):
        return pl.ds(pl.multiple_of(start, size), size)

    def remote(src, dst, ssem, rsem, target):
        return pltpu.make_async_remote_copy(src_ref=src, dst_ref=dst, send_sem=ssem, recv_sem=rsem,
                                            device_id=target, device_id_type=MESH)

    def send(src, dst, ssem, rsem, f):
        remote(src, dst, ssem, rsem, {"fsdp": f}).start()

    def wait_recv(ref, sem):
        remote(ref, ref, sem, sem, {"fsdp": partner}).wait_recv()

    def wait_send(ref, sem):
        remote(ref, ref, sem, sem, {"fsdp": partner}).wait_send()

    b0, b1 = t % 2, t // 2

    def y_plan(cc):
        if cc == 0:
            return t ^ 1, t ^ 3, (b0 + b1) % 2, b1
        return t ^ 3, t ^ 1, b1, b0

    def my_rows(cc):
        _, _, k1, k2 = y_plan(cc)
        return al(k1 * hs + k2 * qs, qs)

    barrier = pltpu.get_barrier_semaphore()
    for d in range(1, 8):
        pl.semaphore_signal(barrier, inc=1, device_id={"fsdp": lax.rem(me + d, n_dev)}, device_id_type=MESH)
    for m in (1, 3):
        pl.semaphore_signal(barrier, inc=1, device_id={"tp": t ^ m}, device_id_type=MESH)
    for f in range(dm // rows):
        pltpu.make_async_copy(x.at[:, pl.ds(f * rows, rows)], ag.at[f], osem.at[0]).start()
    pltpu.make_async_copy(pos, posv, osem.at[1]).start()
    pltpu.make_async_copy(freq, freqv, osem.at[2]).start()
    pltpu.make_async_copy(gain, gl.at[me], osem.at[3]).start()
    pl.semaphore_wait(barrier, 9)

    class Ring:
        def __init__(self, region, own, r, p, s, tp_):
            self.region, self.own, self.r, self.p, self.s, self.t = region, own, r, p, s, tp_

        def own_send(self, ab):
            for way, target, who in ((0, right, LEFT), (1, left, RIGHT)):
                for src, dst in self.own(ab):
                    send(src, dst, self.s.at[way, ab], self.r.at[who - 1, ab], target)
            for src, dst in self.own(ab):
                send(src, dst, self.t.at[OWN, ab], self.p.at[OWN, ab], partner)

        def pass_on(self, r, ab):
            ref = self.region(dev(r, core), ab)
            wait_recv(ref, self.r.at[r - 1, ab])
            send(ref, ref, self.t.at[r, ab], self.p.at[r, ab], partner)

        def service(self):
            for r, ab, target, way in ((LEFT, A, right, 0), (RIGHT, B, left, 1)):
                ref = self.region(dev(r, core), ab)
                wait_recv(ref, self.r.at[r - 1, ab])
                send(ref, ref, self.s.at[way, 2], self.r.at[OPP - 1, ab], target)
                send(ref, ref, self.t.at[r, ab], self.p.at[r, ab], partner)
            self.pass_on(LEFT, B)
            self.pass_on(RIGHT, A)

        def last(self):
            self.pass_on(OPP, A)
            self.pass_on(OPP, B)

        def wait_partner(self, r, ab):
            ref = self.region(dev(r, other), ab)
            wait_recv(ref, self.p.at[r, ab])
            return ref

        def drain(self):
            ref = self.region(0, A)
            for j in range(3):
                for way in (0, 1):
                    wait_send(ref, self.s.at[way, j])
            for r in range(4):
                for ab in (A, B):
                    wait_send(ref, self.t.at[r, ab])

    class Pair:
        def __init__(self, region, own, r, p, s, tp_):
            self.region, self.own, self.r, self.p, self.s, self.t = region, own, r, p, s, tp_

        def one(self, q, side, target, ssem, rsem):
            for src, dst in self.own(lax.rem(chip + q, n_chips), side):
                send(src, dst, ssem, rsem, target)

        def own_first(self):
            self.one(1, 0, right, self.s.at[0, 0], self.r.at[LEFT - 1, 0])
            self.one(2, 1, left, self.s.at[1, 0], self.r.at[RIGHT - 1, 1])

        def own_second(self):
            self.one(0, 1, right, self.s.at[0, 1], self.r.at[LEFT - 1, 1])
            self.one(3, 0, left, self.s.at[1, 1], self.r.at[RIGHT - 1, 0])
            self.one(0, 0, partner, self.t.at[OWN, 0], self.p.at[OWN, 0])
            self.one(3, 1, partner, self.t.at[OWN, 1], self.p.at[OWN, 1])

        def pass_on(self, r, side):
            ref = self.region(dev(r, core), side)
            wait_recv(ref, self.r.at[r - 1, side])
            send(ref, ref, self.t.at[r, side], self.p.at[r, side], partner)

        def forward(self):
            for r, side, target, way in ((LEFT, 0, right, 0), (RIGHT, 1, left, 1)):
                f = dev(r, core)
                ref = self.region(f, side)
                wait_recv(ref, self.r.at[r - 1, side])
                send(ref, self.region(f, 1 - side), self.s.at[way, 2], self.r.at[OPP - 1, 1 - side], target)
                send(ref, ref, self.t.at[r, side], self.p.at[r, side], partner)

        def rest(self):
            self.pass_on(LEFT, 1)
            self.pass_on(RIGHT, 0)

        def last(self):
            self.pass_on(OPP, 0)
            self.pass_on(OPP, 1)

        def wait_partner(self, r, side):
            ref = self.region(dev(r, other), side)
            wait_recv(ref, self.p.at[r, side])
            return ref

        def drain(self):
            ref = self.region(0, 0)
            for j in range(3):
                for way in (0, 1):
                    wait_send(ref, self.s.at[way, j])
            for r in range(4):
                for side in (0, 1):
                    wait_send(ref, self.t.at[r, side])

    half = rows // 2

    def q_region(f, ab):
        return lq.at[f, A, pl.ds(ab * half, half), :]

    qkv = Ring(q_region, lambda ab: ((wq.at[pl.ds(ab * half, half), :], q_region(me, ab)),), rq, pq, sq, tq)

    kv_cols = ((wk, pl.ds(0, hd)), (wv, pl.ds(hd, hd)))
    kv_p1, kv_p2 = t ^ (1 + 2 * core), t ^ (3 - 2 * core)
    kv_k1 = core * b1 + other * lax.rem(b0 + b1, 2)
    kv_k2 = core * b0 + other * b1
    kq = rows // 4
    kv_rows = al(kv_k1 * half + kv_k2 * kq, kq)

    def kv_send():
        for r, who in ((RIGHT, LEFT), (LEFT, RIGHT), (OPP, OPP)):
            for src, cols in kv_cols:
                send(src.at[kv_rows, :], lq.at[me, B, kv_rows, cols], skv.at[r - 1], rkv.at[who - 1], dev(r, core))
        for src, cols in kv_cols:
            send(src, lq.at[me, B, :, cols], tkv.at[OWN], pkv.at[OWN], partner)

    def kv_share(step):
        for r in (RIGHT, OPP, LEFT):
            f = dev(r, core)
            if step == 0:
                ref = lq.at[f, B, kv_rows, :]
                wait_recv(ref, rkv.at[r - 1])
                remote(ref, ref, ska.at[0, r - 1], rka.at[0, r - 1], {"tp": kv_p2}).start()
            elif step == 1:
                wait_recv(lq.at[f, B, al(kv_k1 * half + (1 - kv_k2) * kq, kq), :], rka.at[0, r - 1])
                ref = lq.at[f, B, al(kv_k1 * half, half), :]
                remote(ref, ref, ska.at[1, r - 1], rka.at[1, r - 1], {"tp": kv_p1}).start()
            else:
                wait_recv(lq.at[f, B, al((1 - kv_k1) * half, half), :], rka.at[1, r - 1])
                ref = lq.at[f, B]
                send(ref, ref, tkv.at[r], pkv.at[r], partner)

    def kv_drain():
        for r in range(3):
            wait_send(lq.at[0, B, pl.ds(0, kq), :], skv.at[r])
            wait_send(lq.at[0, B, pl.ds(0, kq), :], ska.at[0, r])
            wait_send(lq.at[0, B, pl.ds(0, half), :], ska.at[1, r])
        for r in range(4):
            wait_send(lq.at[0, B], tkv.at[r])

    def o_own(ab):
        return ((wo.at[pl.ds(ab * (qw // 2), qw // 2), :], lo.at[me, ab]),)

    w_o = Ring(lambda f, ab: lo.at[f, ab], o_own, ro, po, so, to)

    def gu(k):
        def own(q, side):
            cols = al(q * qc + k * kc, kc)
            return ((wg.at[:, cols], lg.at[k, side, me, A]), (wu.at[:, cols], lg.at[k, side, me, B]))

        return Pair(lambda f, side: lg.at[k, side, f], own, rg.at[k], pg.at[k], sg.at[k], tg.at[k])

    def d_own(q, side):
        return ((wd.at[al(q * qc, qc), :], ld.at[me, side]),)

    w_d = Pair(lambda f, side: ld.at[f, side], d_own, rd, pd, sd, td)

    def local(src, dst, sem):
        pltpu.make_async_copy(src, dst, sem).start()

    def finish_qkv():
        qkv.last()
        for src, ab, off, width in ((wq, A, 0, qw), (wk, B, 0, hd), (wv, B, hd, hd)):
            local(src, stg.at[ab, me, :, pl.ds(off, width)], lsem)
        for ab in (A, B):
            for r in (RIGHT, LEFT, OPP):
                f = dev(r, core)
                local(lq.at[f, ab], stg.at[ab, f], lsem)
        for r in (OWN, RIGHT, LEFT, OPP):
            f = dev(r, other)
            for ab in (A, B):
                qkv.wait_partner(r, ab)
            wait_recv(lq.at[f, B], pkv.at[r])
            for ab in (A, B):
                local(lq.at[f, ab], stg.at[ab, f], lsem)
        pltpu.make_async_copy(stg, stg, lsem).wait()

    def finish_gu(k):
        flow = gu(k)

        def stage(r, mine):
            f = dev(r, core if mine else other)
            for side in (0, 1):
                cols = pl.ds(side * kc, kc)
                if not mine:
                    flow.wait_partner(r, side)
                for ab in (A, B):
                    local(lg.at[k, side, f, ab], stg.at[ab, f, :, cols], lsem)

        for side in (0, 1):
            q = lax.rem(chip + 3 * side, n_chips)
            for ab, src in ((A, wg), (B, wu)):
                local(src.at[:, al(q * qc + k * kc, kc)], stg.at[ab, me, :, pl.ds(side * kc, kc)], lsem)
        stage(RIGHT, True)
        stage(LEFT, True)
        stage(OWN, False)
        flow.last()
        stage(OPP, True)
        for r in (RIGHT, LEFT, OPP):
            stage(r, False)
        pltpu.make_async_copy(stg, stg, lsem).wait()

    hc = dm // 2

    def h_cols(cc):
        return pl.ds(cc * hc, hc)

    def rows_out():
        for cc, target in ((0, right), (1, left)):
            send(h.at[my_rows(cc), h_cols(cc)], tr.at[cc], sh.at[cc], rt.at[cc], target)

    def rows_forward():
        for cc, target in ((0, right), (1, left)):
            wait_recv(tr.at[cc], rt.at[cc])
            send(tr.at[cc], h2.at[my_rows(cc), h_cols(cc)], sf.at[cc], rh.at[cc], target)

    def rows_share(step):
        for cc in (0, 1):
            p1, p2, k1, k2 = y_plan(cc)
            if step == 0:
                mine = h2.at[my_rows(cc), h_cols(cc)]
                wait_recv(mine, rh.at[cc])
                remote(mine, mine, sa.at[cc, 0], ra.at[cc, 0], {"tp": p2}).start()
            elif step == 1:
                wait_recv(h2.at[al(k1 * hs + (1 - k2) * qs, qs), h_cols(cc)], ra.at[cc, 0])
                mine = h2.at[al(k1 * hs, hs), h_cols(cc)]
                remote(mine, mine, sa.at[cc, 1], ra.at[cc, 1], {"tp": p1}).start()
            else:
                wait_recv(h2.at[al((1 - k1) * hs, hs), h_cols(cc)], ra.at[cc, 1])

    def norm_tile(i, _):
        rr = al(i * 128, 128)
        blocks = [ag[f, rr, :].astype(jnp.float32) for f in range(dm // rows)]
        mean = sum(jnp.sum(b, axis=-1, keepdims=True) for b in blocks) * (1.0 / dm)
        cent = [b - mean for b in blocks]
        var = sum(jnp.sum(c * c, axis=-1, keepdims=True) for c in cent) * (1.0 / dm)
        scale = lax.rsqrt(var + NORM_EPS)
        for f in range(dm // rows):
            h[rr, f * rows:(f + 1) * rows] = (cent[f] * scale * gl[f]).astype(jnp.bfloat16)
        return _

    def rope_tile(i, _):
        angle = freqv[...] * posv[:, al(i * 128, 128)].astype(jnp.float32)
        cosv[al(i * 128, 128), :] = jnp.transpose(jnp.cos(angle))
        sinv[al(i * 128, 128), :] = jnp.transpose(jnp.sin(angle))
        return _

    def qkv_tile(i, _):
        rr = al(i * MT, MT)
        hm = h[rr, :]
        cs, sn = cosv[rr, :], sinv[rr, :]
        q = dot(hm, stg[A].reshape(dm, qw)).astype(jnp.bfloat16).astype(jnp.float32)
        kv = dot(hm, stg[B].reshape(dm, qw)).astype(jnp.bfloat16)
        for vec, base in ((q[:, :hd], 0), (q[:, hd:], hd), (kv[:, :hd].astype(jnp.float32), 2 * hd)):
            a, b = vec[:, :hd // 2], vec[:, hd // 2:]
            act[rr, base:base + hd // 2] = (a * cs - b * sn).astype(jnp.bfloat16)
            act[rr, base + hd // 2:base + hd] = (b * cs + a * sn).astype(jnp.bfloat16)
        act[rr, 3 * hd:] = kv[:, hd:]
        return _

    def attention(head):
        qb = 256

        def block(i, _):
            rr = al(i * qb, qb)
            s = lax.dot_general(act[rr, head * hd:(head + 1) * hd], act[:, 2 * hd:3 * hd],
                                (((1,), (1,)), ((), ())), preferred_element_type=jnp.float32) * (hd ** -0.5)
            qi = i * qb + lax.broadcasted_iota(jnp.int32, (qb, seq), 0)
            ki = lax.broadcasted_iota(jnp.int32, (qb, seq), 1)
            s = jnp.where(ki <= qi, s, -1e30)
            e = jnp.exp(s - jnp.max(s, axis=-1, keepdims=True))
            p = (e * (1.0 / jnp.sum(e, axis=-1, keepdims=True))).astype(jnp.bfloat16)
            o = dot(p, act[:, 3 * hd:])
            z[rr, 2 * qc + head * hd:2 * qc + (head + 1) * hd] = o.astype(jnp.bfloat16)
            return _

        lax.fori_loop(0, seq // qb, block, 0)

    def gate_up(k, src, dst):
        def tile(i, _):
            rr = al(i * MT, MT)
            hm = src[rr, :]
            g = dot(hm, stg[A].reshape(dm, 2 * kc)).astype(jnp.bfloat16).astype(jnp.float32)
            u = dot(hm, stg[B].reshape(dm, 2 * kc)).astype(jnp.bfloat16).astype(jnp.float32)
            r = (g * jax.nn.sigmoid(g) * u).astype(jnp.bfloat16)
            for side in (0, 1):
                dst[rr, side * qc + k * kc:side * qc + (k + 1) * kc] = r[:, side * kc:(side + 1) * kc]
            return _

        lax.fori_loop(0, seq // MT, tile, 0)

    def unit_f(g, cc):
        return dev(g, core if cc == 0 else other)

    def group_load(g):
        slot = SLOT[g]
        for cc in (0, 1):
            f = unit_f(g, cc)
            cols = pl.ds(cc * rows, rows)
            for side in (0, 1):
                dst = dstg.at[slot, pl.ds(side * qc, qc), cols]
                if g == OWN and cc == 0:
                    local(wd.at[al(lax.rem(chip + 3 * side, n_chips) * qc, qc), :], dst, dsem.at[slot])
                else:
                    if cc == 1:
                        w_d.wait_partner(g, side)
                    local(ld.at[f, side], dst, dsem.at[slot])

    def group_load_o(g):
        slot = SLOT[g]
        for cc in (0, 1):
            f = unit_f(g, cc)
            for ab in (A, B):
                dst = dstg.at[slot, pl.ds(2 * qc + ab * (qw // 2), qw // 2), pl.ds(cc * rows, rows)]
                if g == OWN and cc == 0:
                    local(wo.at[pl.ds(ab * (qw // 2), qw // 2), :], dst, dsem.at[2 + slot])
                else:
                    if cc == 1:
                        w_o.wait_partner(g, ab)
                    local(lo.at[f, ab], dst, dsem.at[2 + slot])

    def group_wait(g, s):
        slot = SLOT[g]
        ref = dstg.at[slot, pl.ds(0, 2 * qc), :] if s else dstg.at[slot, pl.ds(2 * qc, qw), :]
        pltpu.make_async_copy(ref, ref, dsem.at[2 * (1 - s) + slot]).wait()

    def group_part(g, s):
        group_wait(g, s)
        slot = SLOT[g]
        src, depth = ((z, 2 * qc + qw), (z2, 2 * qc))[s]

        def tile(i, _):
            rr = al(i * MT, MT)
            r = dot(src[rr, :], dstg[slot, :depth, :]).astype(jnp.bfloat16)
            for cc in (0, 1):
                part[slot, cc, s, rr, :] = r[:, cc * rows:(cc + 1) * rows]
            return _

        lax.fori_loop(0, seq // MT, tile, 0)
        for cc in (0, 1):
            p1, _, k1, _ = y_plan(cc)
            u = 2 * g + cc
            remote(part.at[slot, cc, s, al((1 - k1) * hs, hs), :], rs1.at[u, s],
                   s_y.at[u, 4 * s], r_y.at[u, 4 * s], {"tp": p1}).start()

    def sum_half(g):
        for cc in (0, 1):
            _, p2, k1, k2 = y_plan(cc)
            u = 2 * g + cc
            wait_recv(rs1.at[u, 1], r_y.at[u, 4])
            wait_recv(rs1.at[u, 0], r_y.at[u, 0])
            s1[u] = (part[SLOT[g], cc, :, al(k1 * hs, hs), :].astype(jnp.float32) + rs1[u].astype(jnp.float32)).astype(jnp.bfloat16)
            remote(s1.at[u, :, al((1 - k2) * qs, qs), :], rs2.at[u], s_y.at[u, 1], r_y.at[u, 1], {"tp": p2}).start()

    def part_free(g):
        for cc in (0, 1):
            for st in (0, 4):
                wait_send(rs1.at[0, 0], s_y.at[2 * g + cc, st])

    def sum_quarter(g):
        for cc in (0, 1):
            _, _, _, k2 = y_plan(cc)
            u = 2 * g + cc
            wait_recv(rs2.at[u], r_y.at[u, 1])
            mine = al(k2 * qs, qs)
            xo[u] = (s1[u, 1, mine, :].astype(jnp.float32) + rs2[u, 1].astype(jnp.float32)).astype(jnp.bfloat16)
            f = unit_f(g, cc)
            send(xo.at[u], xi.at[f], s_x.at[u], r_x.at[f], opposite)

    def close(g):
        for cc in (0, 1):
            _, p2, _, k2 = y_plan(cc)
            u = 2 * g + cc
            f = unit_f(g, cc)
            wait_recv(xi.at[f], r_x.at[f])
            mine = al(k2 * qs, qs)
            tot = s1[u, 0, mine, :].astype(jnp.float32) + rs2[u, 0].astype(jnp.float32) + xi[f].astype(jnp.float32)
            ag[u, my_rows(cc), :] = (xres[u].astype(jnp.float32) + tot).astype(jnp.bfloat16)
            ref = ag.at[u, my_rows(cc), :]
            remote(ref, ref, s_y.at[u, 2], r_y.at[u, 2], {"tp": p2}).start()

    def share_half(g):
        for cc in (0, 1):
            p1, _, k1, k2 = y_plan(cc)
            u = 2 * g + cc
            wait_recv(ag.at[u, al(k1 * hs + (1 - k2) * qs, qs), :], r_y.at[u, 2])
            ref = ag.at[u, al(k1 * hs, hs), :]
            remote(ref, ref, s_y.at[u, 3], r_y.at[u, 3], {"tp": p1}).start()

    def store(g):
        for cc in (0, 1):
            _, _, k1, _ = y_plan(cc)
            u = 2 * g + cc
            wait_recv(ag.at[u, al((1 - k1) * hs, hs), :], r_y.at[u, 3])
            local(ag.at[u], out.at[:, al(unit_f(g, cc) * rows, rows)], osem.at[4])

    for d in range(1, 8):
        f = lax.rem(me + d, n_dev)
        send(gain, gl.at[me], s_gain.at[d - 1], r_gain.at[d - 1], f)
    qkv.own_send(A)
    qkv.own_send(B)
    kv_send()
    pltpu.make_async_copy(ag, ag, osem.at[0]).wait()
    pltpu.make_async_copy(gain, gl.at[me], osem.at[3]).wait()
    for d in range(1, 8):
        wait_recv(gl.at[lax.rem(me + n_dev - d, n_dev)], r_gain.at[d - 1])
    lax.fori_loop(0, seq // 128, norm_tile, 0)
    rows_out()
    qkv.service()
    kv_share(0)
    pltpu.make_async_copy(pos, posv, osem.at[1]).wait()
    pltpu.make_async_copy(freq, freqv, osem.at[2]).wait()
    lax.fori_loop(0, seq // 128, rope_tile, 0)
    kv_share(1)
    rows_forward()
    gu(0).own_first()
    gu(0).own_second()
    gu(1).own_first()
    kv_share(2)
    finish_qkv()
    lax.fori_loop(0, seq // MT, qkv_tile, 0)
    rows_share(0)
    attention(0)
    gu(0).forward()
    gu(1).own_second()
    gu(2).own_first()
    attention(1)
    gu(0).rest()
    rows_share(1)
    finish_gu(0)
    gu(1).forward()
    gu(2).own_second()
    gu(3).own_first()
    gate_up(0, h, z)
    gu(1).rest()
    rows_share(2)
    gu(2).forward()
    gu(3).own_second()
    gate_up(0, h2, z2)
    finish_gu(1)
    gate_up(1, h, z)
    gu(2).rest()
    gate_up(1, h2, z2)
    gu(3).forward()
    w_d.own_first()
    w_d.own_second()
    w_o.own_send(A)
    w_o.own_send(B)
    finish_gu(2)
    gate_up(2, h, z)
    gu(3).rest()
    gate_up(2, h2, z2)
    group_load(OWN)
    group_load_o(OWN)
    for g in range(4):
        for cc in (0, 1):
            local(x.at[my_rows(cc), al(unit_f(g, cc) * rows, rows)], xres.at[2 * g + cc], osem.at[0])
    finish_gu(3)
    gate_up(3, h2, z2)
    group_part(OWN, 1)
    w_d.forward()
    gate_up(3, h, z)
    group_part(OWN, 0)
    w_d.rest()
    group_load(RIGHT)
    group_load(LEFT)
    group_part(RIGHT, 1)
    w_o.service()
    group_load_o(RIGHT)
    group_load_o(LEFT)
    group_part(RIGHT, 0)
    sum_half(OWN)
    part_free(OWN)
    group_part(LEFT, 1)
    group_part(LEFT, 0)
    w_d.last()
    w_o.last()
    group_load(OPP)
    group_load_o(OPP)
    sum_half(RIGHT)
    sum_quarter(OWN)
    sum_half(LEFT)
    part_free(RIGHT)
    group_part(OPP, 1)
    group_part(OPP, 0)
    pltpu.make_async_copy(xres, xres, osem.at[0]).wait()
    sum_quarter(RIGHT)
    sum_quarter(LEFT)
    close(LEFT)
    close(RIGHT)
    sum_half(OPP)
    share_half(LEFT)
    sum_quarter(OPP)
    close(OPP)
    share_half(RIGHT)
    close(OWN)
    share_half(OPP)
    store(LEFT)
    store(RIGHT)
    share_half(OWN)
    store(OPP)
    store(OWN)

    for d in range(1, 8):
        wait_send(gl.at[0], s_gain.at[d - 1])
    for cc in (0, 1):
        wait_send(tr.at[cc], sh.at[cc])
        wait_send(tr.at[cc], sf.at[cc])
        wait_send(h2.at[pl.ds(0, qs), h_cols(0)], sa.at[cc, 0])
        wait_send(h2.at[pl.ds(0, hs), h_cols(0)], sa.at[cc, 1])
    qkv.drain()
    kv_drain()
    w_o.drain()
    w_d.drain()
    for k in range(nk):
        gu(k).drain()
    for u in range(8):
        if u // 2 in (LEFT, OPP):
            wait_send(rs1.at[u, 0], s_y.at[u, 0])
            wait_send(rs1.at[u, 1], s_y.at[u, 4])
        wait_send(rs2.at[u], s_y.at[u, 1])
        wait_send(xo.at[u], s_x.at[u])
        wait_send(ag.at[u, pl.ds(0, qs), :], s_y.at[u, 2])
        wait_send(ag.at[u, pl.ds(0, hs), :], s_y.at[u, 3])
    pltpu.make_async_copy(ag, ag, osem.at[4]).wait()


def solution(mesh):
    row_spec = P(("dp", "fsdp"), None, None)

    def local_layer(hidden, positions, norm_gain, w_query, w_key, w_value, w_gate, w_up, w_out, w_down):
        _, seq, dm = hidden.shape
        rows, qw = w_query.shape
        hd = w_key.shape[1]
        ff = w_gate.shape[1]
        n_dev = dm // rows
        qc = ff // (n_dev // 2)
        kc = qw // 2
        nk = qc // kc
        inv_freq = 10000.0 ** (-jnp.arange(0, hd, 2, dtype=jnp.float32) / hd)
        bf, f32 = jnp.bfloat16, jnp.float32
        dma = pltpu.SemaphoreType.DMA
        flow_sems = (dma((3, 2)), dma((4, 2)), dma((2, 3)), dma((4, 2)))
        dims = (seq, dm, rows, qw, hd, ff, qc, kc)
        anyspec = pl.BlockSpec(memory_space=pl.ANY)
        out = pl.pallas_call(
            functools.partial(layer_kernel, dims),
            out_shape=(jax.ShapeDtypeStruct((seq, dm), bf),
                       jax.ShapeDtypeStruct((n_dev, 2, rows, qw), bf),
                       jax.ShapeDtypeStruct((nk, 2, n_dev, 2, rows, kc), bf),
                       jax.ShapeDtypeStruct((n_dev, 2, qc, rows), bf),
                       jax.ShapeDtypeStruct((n_dev, 2, qw // 2, rows), bf)),
            in_specs=[anyspec] * 11,
            out_specs=(anyspec,) * 5,
            scratch_shapes=[
                pltpu.VMEM((seq, dm), bf),
                pltpu.VMEM((seq, dm), bf),
                pltpu.VMEM((seq, 2 * qc + qw), bf),
                pltpu.VMEM((seq, 2 * qc), bf),
                pltpu.VMEM((2, n_dev, rows, qw), bf),
                pltpu.VMEM((seq, 4 * hd), bf),
                pltpu.VMEM((1, seq), jnp.int32),
                pltpu.VMEM((hd // 2, 1), f32),
                pltpu.VMEM((seq, hd // 2), f32),
                pltpu.VMEM((seq, hd // 2), f32),
                pltpu.VMEM((n_dev, 1, rows), f32),
                pltpu.VMEM((2, seq // 4, dm // 2), bf),
                pltpu.VMEM((2, 2 * qc + qw, 2 * rows), bf),
                pltpu.VMEM((2, 2, 2, seq, rows), bf),
                pltpu.VMEM((8, 2, seq // 2, rows), bf),
                pltpu.VMEM((8, 2, seq // 2, rows), bf),
                pltpu.VMEM((8, 2, seq // 4, rows), bf),
                pltpu.VMEM((8, seq // 4, rows), bf),
                pltpu.VMEM((8, seq // 4, rows), bf),
                pltpu.VMEM((8, seq // 4, rows), bf),
                pltpu.VMEM((8, seq, rows), bf),
                *flow_sems,
                dma((3,)), dma((4,)), dma((3,)), dma((4,)), dma((2, 3)), dma((2, 3)),
                dma((nk, 3, 2)), dma((nk, 4, 2)), dma((nk, 2, 3)), dma((nk, 4, 2)),
                *flow_sems,
                *flow_sems,
                *[dma((2,))] * 4, *[dma((2, 2))] * 2,
                dma((8, 5)), dma((8, 5)), dma((8,)), dma((8,)), dma((7,)), dma((7,)),
                dma, dma((4,)), dma((5,)),
            ],
            compiler_params=pltpu.CompilerParams(collective_id=0, has_side_effects=True,
                                                 vmem_limit_bytes=67043328),
        )(hidden.reshape(seq, dm), norm_gain.reshape(1, rows), positions.reshape(1, seq), inv_freq.reshape(hd // 2, 1),
          w_query, w_key, w_value, w_gate, w_up, w_out, w_down)[0]
        return out.reshape(hidden.shape)

    in_specs = (row_spec, P(None), P("fsdp"), P("fsdp", "tp"), P("fsdp", None), P("fsdp", None), P("fsdp", "tp"), P("fsdp", "tp"), P("tp", "fsdp"), P("tp", "fsdp"))
    return jax.shard_map(local_layer, mesh=mesh, in_specs=in_specs, out_specs=row_spec, check_vma=False)
```

```python
import functools

import jax
import jax.numpy as jnp
from jax import lax
from jax.experimental import pallas as pl
from jax.experimental.pallas import tpu as pltpu
from jax.sharding import PartitionSpec as P

NORM_EPS = 1e-6
MESH = pl.DeviceIdType.MESH
A, B = 0, 1
OWN, RIGHT, OPP, LEFT = 0, 1, 2, 3
MT = 512
SLOT = {OWN: 0, RIGHT: 1, LEFT: 0, OPP: 1}


def dot(a, b):
    return jnp.dot(a, b, preferred_element_type=jnp.float32)


def layer_kernel(dims, x, gain, pos, freq, wq, wk, wv, wg, wu, wo, wd,
                 out, lq, lg, ld, lo,
                 h, h2, z, z2, stg, act, posv, freqv, cosv, sinv, gl, tr, dstg, part, rs1, s1, rs2, xo, xi, xres, ag,
                 rq, pq, sq, tq, rkv, pkv, skv, tkv, rka, ska, rg, pg, sg, tg, rd, pd, sd, td, ro, po, so, to,
                 sh, rt, sf, rh, sa, ra, r_y, s_y, r_x, s_x, r_gain, s_gain, lsem, dsem, osem):
    seq, dm, rows, qw, hd, ff, qc, kc = dims
    nk = qc // kc
    hs, qs = seq // 2, seq // 4
    n_dev = lax.axis_size("fsdp")
    n_chips = n_dev // 2
    me = lax.axis_index("fsdp")
    t = lax.axis_index("tp")
    chip, core = me // 2, me % 2
    other = 1 - core

    def dev(r, c):
        return 2 * lax.rem(chip + r, n_chips) + c

    right, left, partner, opposite = dev(RIGHT, core), dev(LEFT, core), dev(OWN, other), dev(OPP, core)

    def al(start, size):
        return pl.ds(pl.multiple_of(start, size), size)

    def remote(src, dst, ssem, rsem, target):
        return pltpu.make_async_remote_copy(src_ref=src, dst_ref=dst, send_sem=ssem, recv_sem=rsem,
                                            device_id=target, device_id_type=MESH)

    def send(src, dst, ssem, rsem, f):
        remote(src, dst, ssem, rsem, {"fsdp": f}).start()

    def wait_recv(ref, sem):
        remote(ref, ref, sem, sem, {"fsdp": partner}).wait_recv()

    def wait_send(ref, sem):
        remote(ref, ref, sem, sem, {"fsdp": partner}).wait_send()

    b0, b1 = t % 2, t // 2

    def y_plan(cc):
        if cc == 0:
            return t ^ 1, t ^ 3, (b0 + b1) % 2, b1
        return t ^ 3, t ^ 1, b1, b0

    def my_rows(cc):
        _, _, k1, k2 = y_plan(cc)
        return al(k1 * hs + k2 * qs, qs)

    barrier = pltpu.get_barrier_semaphore()
    for d in range(1, 8):
        pl.semaphore_signal(barrier, inc=1, device_id={"fsdp": lax.rem(me + d, n_dev)}, device_id_type=MESH)
    for m in (1, 3):
        pl.semaphore_signal(barrier, inc=1, device_id={"tp": t ^ m}, device_id_type=MESH)
    for f in range(dm // rows):
        pltpu.make_async_copy(x.at[:, pl.ds(f * rows, rows)], ag.at[f], osem.at[0]).start()
    pltpu.make_async_copy(pos, posv, osem.at[1]).start()
    pltpu.make_async_copy(freq, freqv, osem.at[2]).start()
    pltpu.make_async_copy(gain, gl.at[me], osem.at[3]).start()
    pl.semaphore_wait(barrier, 9)

    class Ring:
        def __init__(self, region, own, r, p, s, tp_):
            self.region, self.own, self.r, self.p, self.s, self.t = region, own, r, p, s, tp_

        def own_send(self, ab):
            for way, target, who in ((0, right, LEFT), (1, left, RIGHT)):
                for src, dst in self.own(ab):
                    send(src, dst, self.s.at[way, ab], self.r.at[who - 1, ab], target)
            for src, dst in self.own(ab):
                send(src, dst, self.t.at[OWN, ab], self.p.at[OWN, ab], partner)

        def pass_on(self, r, ab):
            ref = self.region(dev(r, core), ab)
            wait_recv(ref, self.r.at[r - 1, ab])
            send(ref, ref, self.t.at[r, ab], self.p.at[r, ab], partner)

        def service(self):
            for r, ab, target, way in ((LEFT, A, right, 0), (RIGHT, B, left, 1)):
                ref = self.region(dev(r, core), ab)
                wait_recv(ref, self.r.at[r - 1, ab])
                send(ref, ref, self.s.at[way, 2], self.r.at[OPP - 1, ab], target)
                send(ref, ref, self.t.at[r, ab], self.p.at[r, ab], partner)
            self.pass_on(LEFT, B)
            self.pass_on(RIGHT, A)

        def last(self):
            self.pass_on(OPP, A)
            self.pass_on(OPP, B)

        def wait_partner(self, r, ab):
            ref = self.region(dev(r, other), ab)
            wait_recv(ref, self.p.at[r, ab])
            return ref

        def drain(self):
            ref = self.region(0, A)
            for j in range(3):
                for way in (0, 1):
                    wait_send(ref, self.s.at[way, j])
            for r in range(4):
                for ab in (A, B):
                    wait_send(ref, self.t.at[r, ab])

    class Pair:
        def __init__(self, region, own, r, p, s, tp_):
            self.region, self.own, self.r, self.p, self.s, self.t = region, own, r, p, s, tp_

        def one(self, q, side, target, ssem, rsem):
            for src, dst in self.own(lax.rem(chip + q, n_chips), side):
                send(src, dst, ssem, rsem, target)

        def own_first(self):
            self.one(1, 0, right, self.s.at[0, 0], self.r.at[LEFT - 1, 0])
            self.one(2, 1, left, self.s.at[1, 0], self.r.at[RIGHT - 1, 1])

        def own_second(self):
            self.one(0, 1, right, self.s.at[0, 1], self.r.at[LEFT - 1, 1])
            self.one(3, 0, left, self.s.at[1, 1], self.r.at[RIGHT - 1, 0])
            self.one(0, 0, partner, self.t.at[OWN, 0], self.p.at[OWN, 0])
            self.one(3, 1, partner, self.t.at[OWN, 1], self.p.at[OWN, 1])

        def pass_on(self, r, side):
            ref = self.region(dev(r, core), side)
            wait_recv(ref, self.r.at[r - 1, side])
            send(ref, ref, self.t.at[r, side], self.p.at[r, side], partner)

        def forward(self):
            for r, side, target, way in ((LEFT, 0, right, 0), (RIGHT, 1, left, 1)):
                f = dev(r, core)
                ref = self.region(f, side)
                wait_recv(ref, self.r.at[r - 1, side])
                send(ref, self.region(f, 1 - side), self.s.at[way, 2], self.r.at[OPP - 1, 1 - side], target)
                send(ref, ref, self.t.at[r, side], self.p.at[r, side], partner)

        def rest(self):
            self.pass_on(LEFT, 1)
            self.pass_on(RIGHT, 0)

        def last(self):
            self.pass_on(OPP, 0)
            self.pass_on(OPP, 1)

        def wait_partner(self, r, side):
            ref = self.region(dev(r, other), side)
            wait_recv(ref, self.p.at[r, side])
            return ref

        def drain(self):
            ref = self.region(0, 0)
            for j in range(3):
                for way in (0, 1):
                    wait_send(ref, self.s.at[way, j])
            for r in range(4):
                for side in (0, 1):
                    wait_send(ref, self.t.at[r, side])

    half = rows // 2

    def q_region(f, ab):
        return lq.at[f, A, pl.ds(ab * half, half), :]

    qkv = Ring(q_region, lambda ab: ((wq.at[pl.ds(ab * half, half), :], q_region(me, ab)),), rq, pq, sq, tq)

    kv_cols = ((wk, pl.ds(0, hd)), (wv, pl.ds(hd, hd)))
    kv_p1, kv_p2 = t ^ (1 + 2 * core), t ^ (3 - 2 * core)
    kv_k1 = core * b1 + other * lax.rem(b0 + b1, 2)
    kv_k2 = core * b0 + other * b1
    kq = rows // 4
    kv_rows = al(kv_k1 * half + kv_k2 * kq, kq)

    def kv_send():
        for r, who in ((RIGHT, LEFT), (LEFT, RIGHT), (OPP, OPP)):
            for src, cols in kv_cols:
                send(src.at[kv_rows, :], lq.at[me, B, kv_rows, cols], skv.at[r - 1], rkv.at[who - 1], dev(r, core))
        for src, cols in kv_cols:
            send(src, lq.at[me, B, :, cols], tkv.at[OWN], pkv.at[OWN], partner)

    def kv_share(step):
        for r in (RIGHT, OPP, LEFT):
            f = dev(r, core)
            if step == 0:
                ref = lq.at[f, B, kv_rows, :]
                wait_recv(ref, rkv.at[r - 1])
                remote(ref, ref, ska.at[0, r - 1], rka.at[0, r - 1], {"tp": kv_p2}).start()
            elif step == 1:
                wait_recv(lq.at[f, B, al(kv_k1 * half + (1 - kv_k2) * kq, kq), :], rka.at[0, r - 1])
                ref = lq.at[f, B, al(kv_k1 * half, half), :]
                remote(ref, ref, ska.at[1, r - 1], rka.at[1, r - 1], {"tp": kv_p1}).start()
            else:
                wait_recv(lq.at[f, B, al((1 - kv_k1) * half, half), :], rka.at[1, r - 1])
                ref = lq.at[f, B]
                send(ref, ref, tkv.at[r], pkv.at[r], partner)

    def kv_drain():
        for r in range(3):
            wait_send(lq.at[0, B, pl.ds(0, kq), :], skv.at[r])
            wait_send(lq.at[0, B, pl.ds(0, kq), :], ska.at[0, r])
            wait_send(lq.at[0, B, pl.ds(0, half), :], ska.at[1, r])
        for r in range(4):
            wait_send(lq.at[0, B], tkv.at[r])

    def o_own(ab):
        return ((wo.at[pl.ds(ab * (qw // 2), qw // 2), :], lo.at[me, ab]),)

    w_o = Ring(lambda f, ab: lo.at[f, ab], o_own, ro, po, so, to)

    def gu(k):
        def own(q, side):
            cols = al(q * qc + k * kc, kc)
            return ((wg.at[:, cols], lg.at[k, side, me, A]), (wu.at[:, cols], lg.at[k, side, me, B]))

        return Pair(lambda f, side: lg.at[k, side, f], own, rg.at[k], pg.at[k], sg.at[k], tg.at[k])

    def d_own(q, side):
        return ((wd.at[al(q * qc, qc), :], ld.at[me, side]),)

    w_d = Pair(lambda f, side: ld.at[f, side], d_own, rd, pd, sd, td)

    def local(src, dst, sem):
        pltpu.make_async_copy(src, dst, sem).start()

    def finish_qkv():
        qkv.last()
        for src, ab, off, width in ((wq, A, 0, qw), (wk, B, 0, hd), (wv, B, hd, hd)):
            local(src, stg.at[ab, me, :, pl.ds(off, width)], lsem)
        for ab in (A, B):
            for r in (RIGHT, LEFT, OPP):
                f = dev(r, core)
                local(lq.at[f, ab], stg.at[ab, f], lsem)
        for r in (OWN, RIGHT, LEFT, OPP):
            f = dev(r, other)
            for ab in (A, B):
                qkv.wait_partner(r, ab)
            wait_recv(lq.at[f, B], pkv.at[r])
            for ab in (A, B):
                local(lq.at[f, ab], stg.at[ab, f], lsem)
        pltpu.make_async_copy(stg, stg, lsem).wait()

    def finish_gu(k):
        flow = gu(k)

        def stage(r, mine):
            f = dev(r, core if mine else other)
            for side in (0, 1):
                cols = pl.ds(side * kc, kc)
                if not mine:
                    flow.wait_partner(r, side)
                for ab in (A, B):
                    local(lg.at[k, side, f, ab], stg.at[ab, f, :, cols], lsem)

        for side in (0, 1):
            q = lax.rem(chip + 3 * side, n_chips)
            for ab, src in ((A, wg), (B, wu)):
                local(src.at[:, al(q * qc + k * kc, kc)], stg.at[ab, me, :, pl.ds(side * kc, kc)], lsem)
        stage(RIGHT, True)
        stage(LEFT, True)
        stage(OWN, False)
        flow.last()
        stage(OPP, True)
        for r in (RIGHT, LEFT, OPP):
            stage(r, False)
        pltpu.make_async_copy(stg, stg, lsem).wait()

    hc = dm // 2

    def h_cols(cc):
        return pl.ds(cc * hc, hc)

    def rows_out():
        for cc, target in ((0, right), (1, left)):
            send(h.at[my_rows(cc), h_cols(cc)], tr.at[cc], sh.at[cc], rt.at[cc], target)

    def rows_forward():
        for cc, target in ((0, right), (1, left)):
            wait_recv(tr.at[cc], rt.at[cc])
            send(tr.at[cc], h2.at[my_rows(cc), h_cols(cc)], sf.at[cc], rh.at[cc], target)

    def rows_share(step):
        for cc in (0, 1):
            p1, p2, k1, k2 = y_plan(cc)
            if step == 0:
                mine = h2.at[my_rows(cc), h_cols(cc)]
                wait_recv(mine, rh.at[cc])
                remote(mine, mine, sa.at[cc, 0], ra.at[cc, 0], {"tp": p2}).start()
            elif step == 1:
                wait_recv(h2.at[al(k1 * hs + (1 - k2) * qs, qs), h_cols(cc)], ra.at[cc, 0])
                mine = h2.at[al(k1 * hs, hs), h_cols(cc)]
                remote(mine, mine, sa.at[cc, 1], ra.at[cc, 1], {"tp": p1}).start()
            else:
                wait_recv(h2.at[al((1 - k1) * hs, hs), h_cols(cc)], ra.at[cc, 1])

    def norm_tile(i, _):
        rr = al(i * 128, 128)
        blocks = [ag[f, rr, :].astype(jnp.float32) for f in range(dm // rows)]
        mean = sum(jnp.sum(b, axis=-1, keepdims=True) for b in blocks) * (1.0 / dm)
        cent = [b - mean for b in blocks]
        var = sum(jnp.sum(c * c, axis=-1, keepdims=True) for c in cent) * (1.0 / dm)
        scale = lax.rsqrt(var + NORM_EPS)
        for f in range(dm // rows):
            h[rr, f * rows:(f + 1) * rows] = (cent[f] * scale * gl[f]).astype(jnp.bfloat16)
        return _

    def rope_tile(i, _):
        angle = freqv[...] * posv[:, al(i * 128, 128)].astype(jnp.float32)
        cosv[al(i * 128, 128), :] = jnp.transpose(jnp.cos(angle))
        sinv[al(i * 128, 128), :] = jnp.transpose(jnp.sin(angle))
        return _

    def qkv_tile(i, _):
        rr = al(i * MT, MT)
        hm = h[rr, :]
        cs, sn = cosv[rr, :], sinv[rr, :]
        q = dot(hm, stg[A].reshape(dm, qw)).astype(jnp.bfloat16).astype(jnp.float32)
        kv = dot(hm, stg[B].reshape(dm, qw)).astype(jnp.bfloat16)
        for vec, base in ((q[:, :hd], 0), (q[:, hd:], hd), (kv[:, :hd].astype(jnp.float32), 2 * hd)):
            a, b = vec[:, :hd // 2], vec[:, hd // 2:]
            act[rr, base:base + hd // 2] = (a * cs - b * sn).astype(jnp.bfloat16)
            act[rr, base + hd // 2:base + hd] = (b * cs + a * sn).astype(jnp.bfloat16)
        act[rr, 3 * hd:] = kv[:, hd:]
        return _

    def attention(head):
        qb = 256

        def block(i, _):
            rr = al(i * qb, qb)
            s = lax.dot_general(act[rr, head * hd:(head + 1) * hd], act[:, 2 * hd:3 * hd],
                                (((1,), (1,)), ((), ())), preferred_element_type=jnp.float32) * (hd ** -0.5)
            qi = i * qb + lax.broadcasted_iota(jnp.int32, (qb, seq), 0)
            ki = lax.broadcasted_iota(jnp.int32, (qb, seq), 1)
            s = jnp.where(ki <= qi, s, -1e30)
            e = jnp.exp(s - jnp.max(s, axis=-1, keepdims=True))
            p = (e * (1.0 / jnp.sum(e, axis=-1, keepdims=True))).astype(jnp.bfloat16)
            o = dot(p, act[:, 3 * hd:])
            z[rr, 2 * qc + head * hd:2 * qc + (head + 1) * hd] = o.astype(jnp.bfloat16)
            return _

        lax.fori_loop(0, seq // qb, block, 0)

    def gate_up(k, src, dst):
        def tile(i, _):
            rr = al(i * MT, MT)
            hm = src[rr, :]
            g = dot(hm, stg[A].reshape(dm, 2 * kc)).astype(jnp.bfloat16).astype(jnp.float32)
            u = dot(hm, stg[B].reshape(dm, 2 * kc)).astype(jnp.bfloat16).astype(jnp.float32)
            r = (g * jax.nn.sigmoid(g) * u).astype(jnp.bfloat16)
            for side in (0, 1):
                dst[rr, side * qc + k * kc:side * qc + (k + 1) * kc] = r[:, side * kc:(side + 1) * kc]
            return _

        lax.fori_loop(0, seq // MT, tile, 0)

    def unit_f(g, cc):
        return dev(g, core if cc == 0 else other)

    def group_load(g):
        slot = SLOT[g]
        for cc in (0, 1):
            f = unit_f(g, cc)
            cols = pl.ds(cc * rows, rows)
            for side in (0, 1):
                dst = dstg.at[slot, pl.ds(side * qc, qc), cols]
                if g == OWN and cc == 0:
                    local(wd.at[al(lax.rem(chip + 3 * side, n_chips) * qc, qc), :], dst, dsem.at[slot])
                else:
                    if cc == 1:
                        w_d.wait_partner(g, side)
                    local(ld.at[f, side], dst, dsem.at[slot])

    def group_load_o(g):
        slot = SLOT[g]
        for cc in (0, 1):
            f = unit_f(g, cc)
            for ab in (A, B):
                dst = dstg.at[slot, pl.ds(2 * qc + ab * (qw // 2), qw // 2), pl.ds(cc * rows, rows)]
                if g == OWN and cc == 0:
                    local(wo.at[pl.ds(ab * (qw // 2), qw // 2), :], dst, dsem.at[2 + slot])
                else:
                    if cc == 1:
                        w_o.wait_partner(g, ab)
                    local(lo.at[f, ab], dst, dsem.at[2 + slot])

    def group_wait(g, s):
        slot = SLOT[g]
        ref = dstg.at[slot, pl.ds(0, 2 * qc), :] if s else dstg.at[slot, pl.ds(2 * qc, qw), :]
        pltpu.make_async_copy(ref, ref, dsem.at[2 * (1 - s) + slot]).wait()

    def group_part(g, s):
        group_wait(g, s)
        slot = SLOT[g]
        src, depth = ((z, 2 * qc + qw), (z2, 2 * qc))[s]

        def tile(i, _):
            rr = al(i * MT, MT)
            r = dot(src[rr, :], dstg[slot, :depth, :]).astype(jnp.bfloat16)
            for cc in (0, 1):
                part[slot, cc, s, rr, :] = r[:, cc * rows:(cc + 1) * rows]
            return _

        lax.fori_loop(0, seq // MT, tile, 0)
        for cc in (0, 1):
            p1, _, k1, _ = y_plan(cc)
            u = 2 * g + cc
            remote(part.at[slot, cc, s, al((1 - k1) * hs, hs), :], rs1.at[u, s],
                   s_y.at[u, 4 * s], r_y.at[u, 4 * s], {"tp": p1}).start()

    def sum_half(g):
        for cc in (0, 1):
            _, p2, k1, k2 = y_plan(cc)
            u = 2 * g + cc
            wait_recv(rs1.at[u, 1], r_y.at[u, 4])
            wait_recv(rs1.at[u, 0], r_y.at[u, 0])
            s1[u] = (part[SLOT[g], cc, :, al(k1 * hs, hs), :].astype(jnp.float32) + rs1[u].astype(jnp.float32)).astype(jnp.bfloat16)
            remote(s1.at[u, :, al((1 - k2) * qs, qs), :], rs2.at[u], s_y.at[u, 1], r_y.at[u, 1], {"tp": p2}).start()

    def part_free(g):
        for cc in (0, 1):
            for st in (0, 4):
                wait_send(rs1.at[0, 0], s_y.at[2 * g + cc, st])

    def sum_quarter(g):
        for cc in (0, 1):
            _, _, _, k2 = y_plan(cc)
            u = 2 * g + cc
            wait_recv(rs2.at[u], r_y.at[u, 1])
            mine = al(k2 * qs, qs)
            xo[u] = (s1[u, 1, mine, :].astype(jnp.float32) + rs2[u, 1].astype(jnp.float32)).astype(jnp.bfloat16)
            f = unit_f(g, cc)
            send(xo.at[u], xi.at[f], s_x.at[u], r_x.at[f], opposite)

    def close(g):
        for cc in (0, 1):
            _, p2, _, k2 = y_plan(cc)
            u = 2 * g + cc
            f = unit_f(g, cc)
            wait_recv(xi.at[f], r_x.at[f])
            mine = al(k2 * qs, qs)
            tot = s1[u, 0, mine, :].astype(jnp.float32) + rs2[u, 0].astype(jnp.float32) + xi[f].astype(jnp.float32)
            ag[u, my_rows(cc), :] = (xres[u].astype(jnp.float32) + tot).astype(jnp.bfloat16)
            ref = ag.at[u, my_rows(cc), :]
            remote(ref, ref, s_y.at[u, 2], r_y.at[u, 2], {"tp": p2}).start()

    def share_half(g):
        for cc in (0, 1):
            p1, _, k1, k2 = y_plan(cc)
            u = 2 * g + cc
            wait_recv(ag.at[u, al(k1 * hs + (1 - k2) * qs, qs), :], r_y.at[u, 2])
            ref = ag.at[u, al(k1 * hs, hs), :]
            remote(ref, ref, s_y.at[u, 3], r_y.at[u, 3], {"tp": p1}).start()

    def store(g):
        for cc in (0, 1):
            _, _, k1, _ = y_plan(cc)
            u = 2 * g + cc
            wait_recv(ag.at[u, al((1 - k1) * hs, hs), :], r_y.at[u, 3])
            local(ag.at[u], out.at[:, al(unit_f(g, cc) * rows, rows)], osem.at[4])

    for d in range(1, 8):
        f = lax.rem(me + d, n_dev)
        send(gain, gl.at[me], s_gain.at[d - 1], r_gain.at[d - 1], f)
    qkv.own_send(A)
    qkv.own_send(B)
    kv_send()
    pltpu.make_async_copy(ag, ag, osem.at[0]).wait()
    pltpu.make_async_copy(gain, gl.at[me], osem.at[3]).wait()
    for d in range(1, 8):
        wait_recv(gl.at[lax.rem(me + n_dev - d, n_dev)], r_gain.at[d - 1])
    lax.fori_loop(0, seq // 128, norm_tile, 0)
    rows_out()
    qkv.service()
    kv_share(0)
    pltpu.make_async_copy(pos, posv, osem.at[1]).wait()
    pltpu.make_async_copy(freq, freqv, osem.at[2]).wait()
    lax.fori_loop(0, seq // 128, rope_tile, 0)
    kv_share(1)
    gu(0).own_first()
    rows_forward()
    gu(0).own_second()
    gu(1).own_first()
    kv_share(2)
    finish_qkv()
    lax.fori_loop(0, seq // MT, qkv_tile, 0)
    rows_share(0)
    attention(0)
    gu(0).forward()
    gu(1).own_second()
    gu(2).own_first()
    attention(1)
    gu(0).rest()
    rows_share(1)
    finish_gu(0)
    gu(1).forward()
    gu(2).own_second()
    gu(3).own_first()
    gate_up(0, h, z)
    gu(1).rest()
    rows_share(2)
    gu(2).forward()
    gu(3).own_second()
    gate_up(0, h2, z2)
    finish_gu(1)
    gate_up(1, h, z)
    gu(2).rest()
    gate_up(1, h2, z2)
    gu(3).forward()
    w_d.own_first()
    w_d.own_second()
    w_o.own_send(A)
    w_o.own_send(B)
    finish_gu(2)
    gate_up(2, h, z)
    gu(3).rest()
    gate_up(2, h2, z2)
    group_load(OWN)
    group_load_o(OWN)
    for g in range(4):
        for cc in (0, 1):
            local(x.at[my_rows(cc), al(unit_f(g, cc) * rows, rows)], xres.at[2 * g + cc], osem.at[0])
    finish_gu(3)
    gate_up(3, h2, z2)
    group_part(OWN, 1)
    w_d.forward()
    gate_up(3, h, z)
    group_part(OWN, 0)
    w_d.rest()
    group_load(RIGHT)
    group_load(LEFT)
    group_part(RIGHT, 1)
    w_o.service()
    group_load_o(RIGHT)
    group_load_o(LEFT)
    group_part(RIGHT, 0)
    sum_half(OWN)
    part_free(OWN)
    group_part(LEFT, 1)
    group_part(LEFT, 0)
    w_d.last()
    w_o.last()
    group_load(OPP)
    group_load_o(OPP)
    sum_half(RIGHT)
    sum_quarter(OWN)
    sum_half(LEFT)
    part_free(RIGHT)
    group_part(OPP, 1)
    group_part(OPP, 0)
    pltpu.make_async_copy(xres, xres, osem.at[0]).wait()
    sum_quarter(RIGHT)
    sum_quarter(LEFT)
    close(LEFT)
    close(RIGHT)
    sum_half(OPP)
    share_half(LEFT)
    sum_quarter(OPP)
    close(OPP)
    share_half(RIGHT)
    close(OWN)
    share_half(OPP)
    store(LEFT)
    store(RIGHT)
    share_half(OWN)
    store(OPP)
    store(OWN)

    for d in range(1, 8):
        wait_send(gl.at[0], s_gain.at[d - 1])
    for cc in (0, 1):
        wait_send(tr.at[cc], sh.at[cc])
        wait_send(tr.at[cc], sf.at[cc])
        wait_send(h2.at[pl.ds(0, qs), h_cols(0)], sa.at[cc, 0])
        wait_send(h2.at[pl.ds(0, hs), h_cols(0)], sa.at[cc, 1])
    qkv.drain()
    kv_drain()
    w_o.drain()
    w_d.drain()
    for k in range(nk):
        gu(k).drain()
    for u in range(8):
        if u // 2 in (LEFT, OPP):
            wait_send(rs1.at[u, 0], s_y.at[u, 0])
            wait_send(rs1.at[u, 1], s_y.at[u, 4])
        wait_send(rs2.at[u], s_y.at[u, 1])
        wait_send(xo.at[u], s_x.at[u])
        wait_send(ag.at[u, pl.ds(0, qs), :], s_y.at[u, 2])
        wait_send(ag.at[u, pl.ds(0, hs), :], s_y.at[u, 3])
    pltpu.make_async_copy(ag, ag, osem.at[4]).wait()


def solution(mesh):
    row_spec = P(("dp", "fsdp"), None, None)

    def local_layer(hidden, positions, norm_gain, w_query, w_key, w_value, w_gate, w_up, w_out, w_down):
        _, seq, dm = hidden.shape
        rows, qw = w_query.shape
        hd = w_key.shape[1]
        ff = w_gate.shape[1]
        n_dev = dm // rows
        qc = ff // (n_dev // 2)
        kc = qw // 2
        nk = qc // kc
        inv_freq = 10000.0 ** (-jnp.arange(0, hd, 2, dtype=jnp.float32) / hd)
        bf, f32 = jnp.bfloat16, jnp.float32
        dma = pltpu.SemaphoreType.DMA
        flow_sems = (dma((3, 2)), dma((4, 2)), dma((2, 3)), dma((4, 2)))
        dims = (seq, dm, rows, qw, hd, ff, qc, kc)
        anyspec = pl.BlockSpec(memory_space=pl.ANY)
        out = pl.pallas_call(
            functools.partial(layer_kernel, dims),
            out_shape=(jax.ShapeDtypeStruct((seq, dm), bf),
                       jax.ShapeDtypeStruct((n_dev, 2, rows, qw), bf),
                       jax.ShapeDtypeStruct((nk, 2, n_dev, 2, rows, kc), bf),
                       jax.ShapeDtypeStruct((n_dev, 2, qc, rows), bf),
                       jax.ShapeDtypeStruct((n_dev, 2, qw // 2, rows), bf)),
            in_specs=[anyspec] * 11,
            out_specs=(anyspec,) * 5,
            scratch_shapes=[
                pltpu.VMEM((seq, dm), bf),
                pltpu.VMEM((seq, dm), bf),
                pltpu.VMEM((seq, 2 * qc + qw), bf),
                pltpu.VMEM((seq, 2 * qc), bf),
                pltpu.VMEM((2, n_dev, rows, qw), bf),
                pltpu.VMEM((seq, 4 * hd), bf),
                pltpu.VMEM((1, seq), jnp.int32),
                pltpu.VMEM((hd // 2, 1), f32),
                pltpu.VMEM((seq, hd // 2), f32),
                pltpu.VMEM((seq, hd // 2), f32),
                pltpu.VMEM((n_dev, 1, rows), f32),
                pltpu.VMEM((2, seq // 4, dm // 2), bf),
                pltpu.VMEM((2, 2 * qc + qw, 2 * rows), bf),
                pltpu.VMEM((2, 2, 2, seq, rows), bf),
                pltpu.VMEM((8, 2, seq // 2, rows), bf),
                pltpu.VMEM((8, 2, seq // 2, rows), bf),
                pltpu.VMEM((8, 2, seq // 4, rows), bf),
                pltpu.VMEM((8, seq // 4, rows), bf),
                pltpu.VMEM((8, seq // 4, rows), bf),
                pltpu.VMEM((8, seq // 4, rows), bf),
                pltpu.VMEM((8, seq, rows), bf),
                *flow_sems,
                dma((3,)), dma((4,)), dma((3,)), dma((4,)), dma((2, 3)), dma((2, 3)),
                dma((nk, 3, 2)), dma((nk, 4, 2)), dma((nk, 2, 3)), dma((nk, 4, 2)),
                *flow_sems,
                *flow_sems,
                *[dma((2,))] * 4, *[dma((2, 2))] * 2,
                dma((8, 5)), dma((8, 5)), dma((8,)), dma((8,)), dma((7,)), dma((7,)),
                dma, dma((4,)), dma((5,)),
            ],
            compiler_params=pltpu.CompilerParams(collective_id=0, has_side_effects=True,
                                                 vmem_limit_bytes=67043328),
        )(hidden.reshape(seq, dm), norm_gain.reshape(1, rows), positions.reshape(1, seq), inv_freq.reshape(hd // 2, 1),
          w_query, w_key, w_value, w_gate, w_up, w_out, w_down)[0]
        return out.reshape(hidden.shape)

    in_specs = (row_spec, P(None), P("fsdp"), P("fsdp", "tp"), P("fsdp", None), P("fsdp", None), P("fsdp", "tp"), P("fsdp", "tp"), P("tp", "fsdp"), P("tp", "fsdp"))
    return jax.shard_map(local_layer, mesh=mesh, in_specs=in_specs, out_specs=row_spec, check_vma=False)
```
